32 devices in a mesh: parts: 2 (over y), shot: 4 (over z), freq: 2 (over x), rep: 2 (over core).
Axes of the slice: x: 2, y: 2, z: 4, core: 2. Of those that a mesh axis runs over, the one named last changes fastest.
Arguments:
- recorded: bfloat16 [2, 4, 2048, 2048], P(None, ('parts', 'freq'), ('shot', 'rep')), parts along dimension 1, may hold values from -6 to 6
- receiver_x: float32 [4096], P('parts'), parts along dimension 0, may hold values from -12800 to 12800
- source_x: float32 [4096], P('parts'), parts along dimension 0, may hold values from -12800 to 12800
Outputs:
- predicted: bfloat16 [2, 4, 2048, 2048], P(None, ('parts', 'freq'), ('shot', 'rep')), parts along dimension 1
The draws below stay inside these ranges and needn't reach their ends.
There are 2 independent parts, one for each index of `parts`. The reference program is written for one: setup_inputs(seed, part) draws one part's arguments, and reference() takes and returns one part's arrays. A program takes and returns all parts, laid end to end along the dimension named above; each array names one. Nothing has to cross between parts.
All inputs are finite; a program needn't handle non-finite values.
Results may differ from the reference program's by a relative error of at most 0.013.
Values may be sent and summed in bfloat16 or wider, within the bound.
A program may use at most 64 MiB of HBM per device.

```python
import math
import jax
import jax.numpy as jnp
from jax import lax

NSRC = 2048
NREC = 2048
NSLOW = 1024
NFREQ = 2


def level_of(stream_key, extent, split, least, high):
    gain, own = 1.0, jax.random.fold_in(stream_key, 6)
    for dim, parts in split:
        heights = jnp.exp(jax.random.uniform(jax.random.fold_in(own, dim), (parts,), jnp.float32, least / len(split), high / len(split)))
        gain = gain * jnp.repeat(heights, extent[dim] // parts).reshape([-1 if axis == dim else 1 for axis in range(len(extent))])
    return gain


def scatter_about(own_key, shape, width, limit, shards=(), kind=jnp.bfloat16):
    values = width * jax.random.normal(own_key, shape, jnp.float32)
    if shards:
        values = values * level_of(own_key, shape, shards, -0.22, 0.18)
    return jnp.clip(values, -limit, limit).astype(kind)


def setup_inputs(seed: int = 0, part: int = 0) -> dict:
    keys = jax.random.split(jax.random.key(seed), 4)
    part_keys = jax.random.split(jax.random.fold_in(keys[3], part), 4)
    return {
        "recorded": scatter_about(part_keys[0], (2, NFREQ, NSRC, NREC), 1.0, 6.0, ((1, 2), (2, 8))),
        "receiver_x": jnp.clip(jax.random.uniform(part_keys[1], (NREC,), jnp.float32, -12800.0, 12800.0), -12800.0, 12800.0),
        "source_x": jnp.clip(jax.random.uniform(part_keys[2], (NSRC,), jnp.float32, -12800.0, 12800.0), -12800.0, 12800.0),
    }


two_pi = 6.283185307179586
base_hertz = 40.0
step_hertz = 0.5
slow_max = 0.0005

def slowness_values(grid_count):
    counts = jnp.arange(grid_count, dtype=jnp.int32)
    return slow_max * ((2 * counts + 1 - grid_count).astype(jnp.float32) / grid_count)

def angle_tables(omegas, positions, slowness_grid):
    phases = (omegas * slowness_grid)[None, :] * positions[:, None]
    return (jnp.cos(phases).astype(jnp.bfloat16), jnp.sin(phases).astype(jnp.bfloat16))

def product(left, right):
    return jnp.dot(left, right, preferred_element_type=jnp.float32)

def reference(recorded, receiver_x, source_x):
    slowness_grid = slowness_values(NSLOW)
    scale_receivers = 1.0 / math.sqrt(NREC)
    scale_sources = 1.0 / math.sqrt(NSRC)
    scale_slices = 1.0 / math.sqrt(NSLOW)

    def one_frequency(inputs):
        index_value, data_real, data_imaginary = inputs
        omegas = two_pi * (base_hertz + step_hertz * index_value)
        receiver_cosine, receiver_sine = angle_tables(omegas, receiver_x, slowness_grid)
        source_cosine, source_sine = angle_tables(omegas, source_x, slowness_grid)
        spread_real = ((product(data_real, receiver_cosine) + product(data_imaginary, receiver_sine)) * scale_receivers).astype(jnp.bfloat16)
        spread_imaginary = ((product(data_imaginary, receiver_cosine) - product(data_real, receiver_sine)) * scale_receivers).astype(jnp.bfloat16)
        plane_real = ((product(source_cosine.T, spread_real) + product(source_sine.T, spread_imaginary)) * scale_sources).astype(jnp.bfloat16)
        plane_imaginary = ((product(source_cosine.T, spread_imaginary) - product(source_sine.T, spread_real)) * scale_sources).astype(jnp.bfloat16)
        multiple_real = ((product(plane_real, plane_real) - product(plane_imaginary, plane_imaginary)) * scale_slices).astype(jnp.bfloat16)
        multiple_imaginary = ((product(plane_real, plane_imaginary) + product(plane_imaginary, plane_real)) * scale_slices).astype(jnp.bfloat16)
        back_real = ((product(source_cosine, multiple_real) - product(source_sine, multiple_imaginary)) * scale_slices).astype(jnp.bfloat16)
        back_imaginary = ((product(source_cosine, multiple_imaginary) + product(source_sine, multiple_real)) * scale_slices).astype(jnp.bfloat16)
        predicted_real = ((product(back_real, receiver_cosine.T) - product(back_imaginary, receiver_sine.T)) * scale_slices).astype(jnp.bfloat16)
        predicted_imaginary = ((product(back_real, receiver_sine.T) + product(back_imaginary, receiver_cosine.T)) * scale_slices).astype(jnp.bfloat16)
        return (predicted_real, predicted_imaginary)
    indices = jnp.arange(NFREQ, dtype=jnp.int32).astype(jnp.float32)
    result_real, result_imaginary = lax.map(one_frequency, (indices, recorded[0], recorded[1]))
    return jnp.stack([result_real, result_imaginary], axis=0)
```

```python
import functools
import math

import jax
import jax.numpy as jnp
from jax import lax
from jax.experimental import pallas as pl
from jax.experimental.pallas import tpu as pltpu
from jax.sharding import PartitionSpec as P

NSLOW = 1024

two_pi = 6.283185307179586
base_hertz = 40.0
step_hertz = 0.5
slow_max = 0.0005
GROUP = ("shot", "rep")


def angle_table(omega, positions):
    half = NSLOW // 2
    fine = math.gcd(half, 16)
    unit = (omega * (slow_max / NSLOW)) * positions
    coarse = (jnp.arange(half // fine, dtype=jnp.int32) * (2 * fine)).astype(jnp.float32)[:, None] * unit
    small = (2 * jnp.arange(fine, dtype=jnp.int32) + 1).astype(jnp.float32)[:, None] * unit
    cos_a, sin_a = jnp.cos(coarse)[:, None], jnp.sin(coarse)[:, None]
    cos_b, sin_b = jnp.cos(small)[None], jnp.sin(small)[None]
    cosine = cos_a * cos_b - sin_a * sin_b
    sine = sin_a * cos_b + cos_a * sin_b
    return jnp.stack([cosine, sine]).astype(jnp.bfloat16).reshape(NSLOW, positions.shape[0])


def product(form, left, right):
    return jnp.einsum(form, left, right, preferred_element_type=jnp.float32)


def one_frequency(data, receiver_x, source_x, omega):
    shots = data.shape[1]
    src_count, rec_count = source_x.shape[0], receiver_x.shape[0]
    receiver = angle_table(omega, receiver_x)
    source = angle_table(omega, source_x)
    first = lax.axis_index(GROUP) * shots
    mine = angle_table(omega, lax.dynamic_slice_in_dim(source_x, first, shots, 0))
    spread = (product("csr,jr->csj", data, receiver) * math.sqrt(2.0 / rec_count)).astype(jnp.bfloat16)
    met = lax.all_to_all(spread, GROUP, split_axis=2, concat_axis=1, tiled=True)
    plane = (product("qs,csj->cqj", source, met) * math.sqrt(2.0 / src_count)).astype(jnp.bfloat16)
    planes = lax.all_gather(plane, GROUP, axis=2, tiled=True)
    sign = jnp.where(jnp.arange(NSLOW) < NSLOW // 2, 1.0, -1.0) * math.sqrt(2.0 / NSLOW)
    half_way = (product("qs,cqj->csj", mine, planes) * sign).astype(jnp.bfloat16)
    back_real = product("sm,mj->sj", half_way[0], planes[0]) - product("sm,mj->sj", half_way[1], planes[1])
    back_imaginary = product("sm,mj->sj", half_way[0], planes[1]) + product("sm,mj->sj", half_way[1], planes[0])
    back = (jnp.stack([back_real, back_imaginary]) * math.sqrt(1.0 / NSLOW)).astype(jnp.bfloat16)
    return (product("csj,jr->csr", back, receiver) * math.sqrt(2.0 / NSLOW)).astype(jnp.bfloat16)


FINE = 16
HALF = NSLOW // 2
COARSE = HALF // FINE
MESH = pl.DeviceIdType.MESH


def fill_factors(omega, positions, factors):
    count = positions.shape[1]
    tile = math.gcd(count, 256)
    sines = [(-1.0) ** n / math.factorial(2 * n + 1) for n in range(7)]
    cosines = [(-1.0) ** n / math.factorial(2 * n) for n in range(8)]
    turn_high = 6.28125
    turn_low = two_pi - turn_high

    def step(i, carry):
        lanes = pl.ds(pl.multiple_of(i * tile, tile), tile)
        unit = positions[:, lanes] * (omega * (slow_max / NSLOW))
        row = lax.broadcasted_iota(jnp.int32, (COARSE + FINE, tile), 0)
        steps = jnp.where(row < COARSE, row * (2 * FINE), 2 * (row - COARSE) + 1).astype(jnp.float32)
        phase = steps * unit
        turns = jnp.floor(phase * (1.0 / two_pi) + 0.5)
        half = 0.5 * ((phase - turns * turn_high) - turns * turn_low)
        square = half * half
        sine, cosine = sines[-1], cosines[-1]
        for term in reversed(sines[:-1]):
            sine = sine * square + term
        for term in reversed(cosines[:-1]):
            cosine = cosine * square + term
        sine = sine * half
        factors[0, :, lanes] = 1.0 - 2.0 * sine * sine
        factors[1, :, lanes] = 2.0 * sine * cosine
        return carry

    lax.fori_loop(0, count // tile, step, 0)


def fill_table(factors, table):
    count = table.shape[1]
    tile = math.gcd(count, 512)
    for first in range(0, count, tile):
        lanes = slice(first, first + tile)
        cos_b = factors[0, COARSE : COARSE + FINE, lanes]
        sin_b = factors[1, COARSE : COARSE + FINE, lanes]

        def step(a, carry):
            cos_a = factors[0, pl.ds(a, 1), lanes]
            sin_a = factors[1, pl.ds(a, 1), lanes]
            row = pl.multiple_of(a * FINE, FINE)
            table[pl.ds(row, FINE), lanes] = (cos_a * cos_b - sin_a * sin_b).astype(jnp.bfloat16)
            table[pl.ds(HALF + row, FINE), lanes] = (sin_a * cos_b + cos_a * sin_b).astype(jnp.bfloat16)
            return carry

        lax.fori_loop(0, COARSE, step, 0, unroll=4)


def dot(left, right):
    return jnp.dot(left, right, preferred_element_type=jnp.float32)


def whole_kernel(
    chips, first_hertz, data_in, receiver_in, source_in, back, receiver,
    data, receiver_x, source_x, source, receiver_f, source_f, mine, outgoing, met, planes, half_way,
    spread_send, spread_recv, plane_send, plane_recv, load_sem,
):
    cores = 2
    group = chips * cores
    width = NSLOW // group
    shots = data.shape[0] // 2
    z, c = lax.axis_index("shot"), lax.axis_index("rep")
    me = z * cores + c
    loads = [
        pltpu.make_async_copy(src, dst, load_sem.at[i])
        for i, (src, dst) in enumerate(((receiver_in, receiver_x), (source_in, source_x), (data_in, data)))
    ]
    for load in loads:
        load.start()

    def place(d):
        return {"shot": d // cores, "rep": d % cores}

    barrier = pltpu.get_barrier_semaphore()
    for d in range(group):
        @pl.when(d != me)
        def _():
            pl.semaphore_signal(barrier, inc=1, device_id=place(d), device_id_type=MESH)

    hertz = first_hertz(lax.axis_index("freq")).astype(jnp.float32)
    omega = two_pi * (base_hertz + step_hertz * hertz)
    loads[0].wait()
    fill_factors(omega, receiver_x, receiver_f)
    fill_table(receiver_f, receiver)
    loads[2].wait()
    pl.semaphore_wait(barrier, group - 1)

    def spread_copy(h, d):
        return pltpu.make_async_remote_copy(
            src_ref=outgoing.at[h, d], dst_ref=met.at[h, pl.ds(pl.multiple_of(me * shots, shots), shots)],
            send_sem=spread_send.at[h, d], recv_sem=spread_recv.at[h, me],
            device_id=place(d), device_id_type=MESH,
        )

    scale = math.sqrt(2.0 / data.shape[1])
    order = sorted(range(1, chips), key=lambda k: abs(2 * k - chips)) + [0]
    for h in range(2):
        for offset in order:
            target = lax.rem(z + offset, chips)
            rows = receiver[pl.ds(pl.multiple_of(target * (cores * width), cores * width), cores * width), :]
            part = lax.dot_general(
                data[h * shots : (h + 1) * shots, :], rows, (((1,), (1,)), ((), ())),
                preferred_element_type=jnp.float32,
            )
            part = (part * scale).astype(jnp.bfloat16)
            for e in range(cores):
                d = target * cores + e
                piece = part[:, e * width : (e + 1) * width]
                if offset == 0:
                    @pl.when(d == me)
                    def _():
                        met[h, pl.ds(pl.multiple_of(me * shots, shots), shots), :] = piece

                    @pl.when(d != me)
                    def _():
                        outgoing[h, d] = piece
                        spread_copy(h, d).start()
                else:
                    outgoing[h, d] = piece
                    spread_copy(h, d).start()

    loads[1].wait()
    fill_factors(omega, source_x, source_f)
    fill_table(source_f, source)
    local = source[:, pl.ds(pl.multiple_of(me * shots, shots), shots)]
    mine[...] = local.T

    def plane_copy(way, h, d):
        to = [{"shot": z + 1, "rep": c}, {"shot": z - 1, "rep": c}, {"shot": z, "rep": 1 - c}][way]
        piece = planes.at[d, :, h * width : (h + 1) * width]
        return pltpu.make_async_remote_copy(
            src_ref=piece, dst_ref=piece, send_sem=plane_send.at[way, h, d], recv_sem=plane_recv.at[h, d],
            device_id=to, device_id_type=MESH,
        )

    scale = math.sqrt(2.0 / source.shape[1])
    tile = 256
    more_up, more_down = z < chips - 1, z > 0
    for h in range(2):
        for d in range(group):
            @pl.when(d != me)
            def _():
                pltpu.make_async_remote_copy(
                    src_ref=outgoing.at[h, d], dst_ref=met.at[h, pl.ds(d * shots, shots)],
                    send_sem=spread_send.at[h, d], recv_sem=spread_recv.at[h, d],
                    device_id=place(d), device_id_type=MESH,
                ).wait_recv()

        def plane_rows(i, carry):
            rows = pl.ds(pl.multiple_of(i * tile, tile), tile)
            piece = (dot(source[rows, :], met[h]) * scale).astype(jnp.bfloat16)
            planes[me, rows, h * width : (h + 1) * width] = piece
            return carry

        lax.fori_loop(0, NSLOW // tile, plane_rows, 0)

        @pl.when(more_up)
        def _():
            plane_copy(0, h, me).start()

        @pl.when(more_down)
        def _():
            plane_copy(1, h, me).start()

        plane_copy(2, h, me).start()

    def half_slice(d):
        sign = (1 - 2 * (d // (group // 2))).astype(jnp.float32)
        part = (dot(mine[...], planes[d]) * math.sqrt(2.0 / NSLOW) * sign).astype(jnp.bfloat16)
        lanes = pl.ds(pl.multiple_of(d * width, width), width)
        half_way[:shots, lanes] = part[:, :width]
        half_way[shots:, lanes] = part[:, width:]

    half_slice(me)
    for k in range(1, chips):
        for h in range(2):
            for way, sign in ((0, -1), (1, 1)):
                origin = z + sign * k

                @pl.when((origin >= 0) & (origin < chips))
                def _():
                    d = origin * cores + c
                    plane_copy(2, h, d).wait_recv()

                    @pl.when((more_up, more_down)[way])
                    def _():
                        plane_copy(way, h, d).start()

                    plane_copy(2, h, d).start()
                    if h == 1:
                        half_slice(d)

        for sign in ((-1, 1) if k > 1 else (1,)):
            origin = z + sign * (k - 1)

            @pl.when((origin >= 0) & (origin < chips))
            def _():
                d = origin * cores + 1 - c
                plane_copy(2, 0, d).wait_recv()
                plane_copy(2, 1, d).wait_recv()
                half_slice(d)

    for sign in (-1, 1):
        origin = z + sign * (chips - 1)

        @pl.when((origin >= 0) & (origin < chips))
        def _():
            d = origin * cores + 1 - c
            plane_copy(2, 0, d).wait_recv()
            plane_copy(2, 1, d).wait_recv()
            half_slice(d)

    scale_back = math.sqrt(1.0 / NSLOW)

    def back_slice(d, carry):
        both = dot(half_way[...], planes[d])
        lanes = pl.ds(pl.multiple_of(d * width, width), width)
        back[:shots, lanes] = ((both[:shots, :width] - both[shots:, width:]) * scale_back).astype(jnp.bfloat16)
        back[shots:, lanes] = ((both[:shots, width:] + both[shots:, :width]) * scale_back).astype(jnp.bfloat16)
        return carry

    lax.fori_loop(0, group, back_slice, 0)
    for h in range(2):
        for d in range(group):
            @pl.when(d != me)
            def _():
                spread_copy(h, d).wait_send()
        plane_copy(2, h, me).wait_send()

        @pl.when(more_up)
        def _():
            plane_copy(0, h, me).wait_send()

        @pl.when(more_down)
        def _():
            plane_copy(1, h, me).wait_send()

        for k in range(1, chips):
            for way, sign in ((0, -1), (1, 1)):
                origin = z + sign * k

                @pl.when((origin >= 0) & (origin < chips))
                def _():
                    d = origin * cores + c

                    @pl.when((more_up, more_down)[way])
                    def _():
                        plane_copy(way, h, d).wait_send()

                    plane_copy(2, h, d).wait_send()


def one_frequency_fused(chips, first_hertz, data, receiver_x, source_x):
    shots, rec_count = data.shape[1:]
    src_count = source_x.shape[0]
    group = 2 * chips
    width = NSLOW // group
    vmem = pl.BlockSpec(memory_space=pltpu.VMEM)
    half = jnp.bfloat16
    back, receiver = pl.pallas_call(
        functools.partial(whole_kernel, chips, first_hertz),
        out_shape=(
            jax.ShapeDtypeStruct((2 * shots, NSLOW), half),
            jax.ShapeDtypeStruct((NSLOW, rec_count), half),
        ),
        in_specs=[pl.BlockSpec(memory_space=pltpu.HBM)] * 3,
        out_specs=(vmem, vmem),
        scratch_shapes=[
            pltpu.VMEM((2 * shots, rec_count), half),
            pltpu.VMEM((1, rec_count), jnp.float32),
            pltpu.VMEM((1, src_count), jnp.float32),
            pltpu.VMEM((NSLOW, src_count), half),
            pltpu.VMEM((2, COARSE + FINE, rec_count), jnp.float32),
            pltpu.VMEM((2, COARSE + FINE, src_count), jnp.float32),
            pltpu.VMEM((shots, NSLOW), half),
            pltpu.VMEM((2, group, shots, width), half),
            pltpu.VMEM((2, src_count, width), half),
            pltpu.VMEM((group, NSLOW, 2 * width), half),
            pltpu.VMEM((2 * shots, NSLOW), half),
            pltpu.SemaphoreType.DMA((2, group)),
            pltpu.SemaphoreType.DMA((2, group)),
            pltpu.SemaphoreType.DMA((3, 2, group)),
            pltpu.SemaphoreType.DMA((2, group)),
            pltpu.SemaphoreType.DMA((3,)),
        ],
        compiler_params=pltpu.CompilerParams(
            collective_id=0, has_side_effects=True, vmem_limit_bytes=26 * 1024 * 1024
        ),
        name="plane_wave_multiples",
    )(*[
        pltpu.with_memory_space_constraint(x, pltpu.HBM)
        for x in (data.reshape(2 * shots, rec_count), receiver_x.reshape(1, rec_count), source_x.reshape(1, src_count))
    ])
    result = (dot(back, receiver) * math.sqrt(2.0 / NSLOW)).astype(half)
    return result.reshape(2, shots, rec_count)


def fits(mesh_shape, shots):
    group = mesh_shape["shot"] * mesh_shape["rep"]
    return mesh_shape["rep"] == 2 and NSLOW % (128 * group) == 0 and shots % 128 == 0


def body(chips, fused, recorded, receiver_x, source_x):
    per_device = recorded.shape[1]
    first_freq = lax.axis_index("freq") * per_device
    outs = []
    for k in range(per_device):
        omega = two_pi * (base_hertz + step_hertz * (first_freq + k).astype(jnp.float32))
        if fused(recorded.shape[2]):
            first_hertz = functools.partial(lambda k, f: f * per_device + k, k)
            outs.append(one_frequency_fused(chips, first_hertz, recorded[:, k], receiver_x, source_x))
        else:
            outs.append(one_frequency(recorded[:, k], receiver_x, source_x, omega))
    return jnp.stack(outs, axis=1)


def solution(mesh):
    return jax.shard_map(
        functools.partial(body, mesh.shape["shot"], functools.partial(fits, mesh.shape)),
        mesh=mesh,
        in_specs=(P(None, ("parts", "freq"), ("shot", "rep"), None), P("parts"), P("parts")),
        out_specs=P(None, ("parts", "freq"), ("shot", "rep"), None),
        check_vma=False,
    )
```

```python
import functools
import math

import jax
import jax.numpy as jnp
from jax import lax
from jax.experimental import pallas as pl
from jax.experimental.pallas import tpu as pltpu
from jax.sharding import PartitionSpec as P

NSLOW = 1024

two_pi = 6.283185307179586
base_hertz = 40.0
step_hertz = 0.5
slow_max = 0.0005
GROUP = ("shot", "rep")


def angle_table(omega, positions):
    half = NSLOW // 2
    fine = math.gcd(half, 16)
    unit = (omega * (slow_max / NSLOW)) * positions
    coarse = (jnp.arange(half // fine, dtype=jnp.int32) * (2 * fine)).astype(jnp.float32)[:, None] * unit
    small = (2 * jnp.arange(fine, dtype=jnp.int32) + 1).astype(jnp.float32)[:, None] * unit
    cos_a, sin_a = jnp.cos(coarse)[:, None], jnp.sin(coarse)[:, None]
    cos_b, sin_b = jnp.cos(small)[None], jnp.sin(small)[None]
    cosine = cos_a * cos_b - sin_a * sin_b
    sine = sin_a * cos_b + cos_a * sin_b
    return jnp.stack([cosine, sine]).astype(jnp.bfloat16).reshape(NSLOW, positions.shape[0])


def product(form, left, right):
    return jnp.einsum(form, left, right, preferred_element_type=jnp.float32)


def one_frequency(data, receiver_x, source_x, omega):
    shots = data.shape[1]
    src_count, rec_count = source_x.shape[0], receiver_x.shape[0]
    receiver = angle_table(omega, receiver_x)
    source = angle_table(omega, source_x)
    first = lax.axis_index(GROUP) * shots
    mine = angle_table(omega, lax.dynamic_slice_in_dim(source_x, first, shots, 0))
    spread = (product("csr,jr->csj", data, receiver) * math.sqrt(2.0 / rec_count)).astype(jnp.bfloat16)
    met = lax.all_to_all(spread, GROUP, split_axis=2, concat_axis=1, tiled=True)
    plane = (product("qs,csj->cqj", source, met) * math.sqrt(2.0 / src_count)).astype(jnp.bfloat16)
    planes = lax.all_gather(plane, GROUP, axis=2, tiled=True)
    sign = jnp.where(jnp.arange(NSLOW) < NSLOW // 2, 1.0, -1.0) * math.sqrt(2.0 / NSLOW)
    half_way = (product("qs,cqj->csj", mine, planes) * sign).astype(jnp.bfloat16)
    back_real = product("sm,mj->sj", half_way[0], planes[0]) - product("sm,mj->sj", half_way[1], planes[1])
    back_imaginary = product("sm,mj->sj", half_way[0], planes[1]) + product("sm,mj->sj", half_way[1], planes[0])
    back = (jnp.stack([back_real, back_imaginary]) * math.sqrt(1.0 / NSLOW)).astype(jnp.bfloat16)
    return (product("csj,jr->csr", back, receiver) * math.sqrt(2.0 / NSLOW)).astype(jnp.bfloat16)


FINE = 16
HALF = NSLOW // 2
COARSE = HALF // FINE
BLOCK = 128
PAIRS = HALF // BLOCK
PIECES = 4
MESH = pl.DeviceIdType.MESH

OWNER = (1, 2, 0, 3, 1, 2, 0, 3)
OWN = tuple(tuple(nb for nb, owner in enumerate(OWNER) if owner == at) for at in range(4))
ORDER = (
    (2, 0, 6, 4, 1, 5, 3, 7),
    (0, 4, 1, 2, 5, 6, 3, 7),
    (1, 5, 0, 3, 4, 7, 2, 6),
    (3, 1, 7, 5, 0, 4, 2, 6),
)
BLOCKS = len(OWNER)


def fill_factors(omega, positions, factors, first, rows):
    count = positions.shape[1]
    tile = math.gcd(count, 256)
    sines = [(-1.0) ** n / math.factorial(2 * n + 1) for n in range(7)]
    cosines = [(-1.0) ** n / math.factorial(2 * n) for n in range(8)]
    turn_high = 6.28125
    turn_low = two_pi - turn_high

    def step(i, carry):
        lanes = pl.ds(pl.multiple_of(i * tile, tile), tile)
        unit = positions[:, lanes] * (omega * (slow_max / NSLOW))
        row = lax.broadcasted_iota(jnp.int32, (rows, tile), 0) + first
        steps = jnp.where(row < FINE, 2 * row + 1, (row - FINE) * (2 * FINE)).astype(jnp.float32)
        phase = steps * unit
        turns = jnp.floor(phase * (1.0 / two_pi) + 0.5)
        half = 0.5 * ((phase - turns * turn_high) - turns * turn_low)
        square = half * half
        sine, cosine = sines[-1], cosines[-1]
        for term in reversed(sines[:-1]):
            sine = sine * square + term
        for term in reversed(cosines[:-1]):
            cosine = cosine * square + term
        sine = sine * half
        factors[0, first : first + rows, lanes] = 1.0 - 2.0 * sine * sine
        factors[1, first : first + rows, lanes] = 2.0 * sine * cosine
        return carry

    lax.fori_loop(0, count // tile, step, 0)


def fill_pair(factors, table, p):
    count = table.shape[1]
    tile = math.gcd(count, 512)
    steps = BLOCK // FINE
    for first in range(0, count, tile):
        lanes = slice(first, first + tile)
        cos_b = factors[0, :FINE, lanes]
        sin_b = factors[1, :FINE, lanes]

        def step(a, carry):
            cos_a = factors[0, pl.ds(FINE + p * steps + a, 1), lanes]
            sin_a = factors[1, pl.ds(FINE + p * steps + a, 1), lanes]
            row = pl.multiple_of(2 * BLOCK * p + a * FINE, FINE)
            table[pl.ds(row, FINE), lanes] = (cos_a * cos_b - sin_a * sin_b).astype(jnp.bfloat16)
            table[pl.ds(row + BLOCK, FINE), lanes] = (sin_a * cos_b + cos_a * sin_b).astype(jnp.bfloat16)
            return carry

        lax.fori_loop(0, steps, step, 0, unroll=4)


def dot(left, right):
    return jnp.dot(left, right, preferred_element_type=jnp.float32)


def whole_kernel(
    first_hertz, data_in, receiver_in, source_in, back, receiver,
    data, receiver_x, source_x, source, receiver_f, source_f, mine, outgoing, met, planes, half_way, total,
    spread_send, spread_recv, plane_send, plane_recv, twin_recv, load_sem,
):
    chips, cores = len(OWN), 2
    group = chips * cores
    shots = data.shape[0] // 2
    z, c = lax.axis_index("shot"), lax.axis_index("rep")
    me = z * cores + c
    side = z // 2
    more_up, more_down = z < chips - 1, z > 0

    def pick(values):
        out = jnp.int32(values[-1])
        for i, value in enumerate(values[:-1]):
            out = jnp.where(z == i, jnp.int32(value), out)
        return out

    packed = pick([sum(nb << (3 * i) for i, nb in enumerate(row)) for row in ORDER])

    def nth(i):
        return lax.rem(packed >> (3 * i), BLOCKS)

    def place(d):
        return {"shot": d // cores, "rep": d % cores}

    loads = [
        pltpu.make_async_copy(src, dst, load_sem.at[i])
        for i, (src, dst) in enumerate(((receiver_in, receiver_x), (data_in, data), (source_in, source_x)))
    ]
    for load in loads:
        load.start()
    barrier = pltpu.get_barrier_semaphore()
    for d in range(group):
        @pl.when(d != me)
        def _():
            pl.semaphore_signal(barrier, inc=1, device_id=place(d), device_id_type=MESH)

    hertz = first_hertz(lax.axis_index("freq")).astype(jnp.float32)
    omega = two_pi * (base_hertz + step_hertz * hertz)
    own_rows = pl.ds(pl.multiple_of(me * shots, shots), shots)

    def spread_copy(p, s, h, to):
        return pltpu.make_async_remote_copy(
            src_ref=outgoing.at[4 * p + 2 * s + h], dst_ref=met.at[p, own_rows],
            send_sem=spread_send, recv_sem=spread_recv.at[p],
            device_id={"shot": to, "rep": h}, device_id_type=MESH,
        )

    def put(p, h, part):
        part = (part * math.sqrt(2.0 / data.shape[1])).astype(jnp.bfloat16)
        for s in range(2):
            piece = part[:, s * BLOCK : (s + 1) * BLOCK]
            here = me == OWNER[2 * p + s] * cores + h

            @pl.when(here)
            def _():
                met[p, own_rows, :] = piece

            @pl.when(jnp.logical_not(here))
            def _():
                outgoing[4 * p + 2 * s + h] = piece

    def send(p, h):
        for k in range(2):
            s = lax.rem(1 - side + c + k, 2)
            to = jnp.where(s == 0, OWNER[2 * p], OWNER[2 * p + 1])

            @pl.when((to != z) | (c != h))
            def _():
                spread_copy(p, s, h, to).start()

    def spread(p, rows):
        return lax.dot_general(
            data[rows, :], receiver[2 * BLOCK * p : 2 * BLOCK * (p + 1), :], (((1,), (1,)), ((), ())),
            preferred_element_type=jnp.float32,
        )

    loads[0].wait()
    first_rows = FINE + BLOCK // FINE
    fill_factors(omega, receiver_x, receiver_f, 0, first_rows)
    fill_pair(receiver_f, receiver, 0)
    loads[1].wait()
    for h in range(2):
        put(0, h, spread(0, slice(h * shots, (h + 1) * shots)))
        if h == 0:
            pl.semaphore_wait(barrier, group - 1)
        send(0, h)
    fill_factors(omega, receiver_x, receiver_f, first_rows, FINE + COARSE - first_rows)
    for p in range(1, PAIRS):
        fill_pair(receiver_f, receiver, p)
        part = spread(p, slice(0, 2 * shots))
        for h in range(2):
            put(p, h, part[h * shots : (h + 1) * shots])
        for h in range(2):
            send(p, h)

    loads[2].wait()
    fill_factors(omega, source_x, source_f, 0, FINE + COARSE)
    for p in range(PAIRS):
        fill_pair(source_f, source, p)
    mine[...] = source[:, own_rows].T
    half_way[...] = jnp.zeros_like(half_way)

    rows_of = NSLOW // PIECES

    def plane_copy(way, nb, h, piece):
        to = [{"shot": z + 1, "rep": c}, {"shot": z - 1, "rep": c}, {"shot": z, "rep": 1 - c}][way]
        part = planes.at[nb, h, pl.ds(pl.multiple_of(piece * rows_of, rows_of), rows_of)]
        return pltpu.make_async_remote_copy(
            src_ref=part, dst_ref=part, send_sem=plane_send.at[way],
            recv_sem=twin_recv.at[nb] if way == 2 else plane_recv.at[nb, piece],
            device_id=to, device_id_type=MESH,
        )

    def whole_copy(way, blocks, recv_sem):
        part = planes.at[blocks, 0]
        return pltpu.make_async_remote_copy(
            src_ref=part, dst_ref=part, send_sem=plane_send.at[way], recv_sem=recv_sem,
            device_id={"rep": 1 - c}, device_id_type=MESH,
        )

    def each_way(nb, up, down, piece, act):
        @pl.when(up)
        def _():
            act(plane_copy(0, nb, c, piece))

        @pl.when(down)
        def _():
            act(plane_copy(1, nb, c, piece))

        act(plane_copy(2, nb, c, piece))

    def start(copy):
        copy.start()

    def own_slice(nb):
        p = nb // 2
        arrived = met.at[p, pl.ds(0, (group - 1) * shots)]
        pltpu.make_async_remote_copy(
            src_ref=arrived, dst_ref=arrived, send_sem=spread_send, recv_sem=spread_recv.at[p],
            device_id={"rep": 1 - c}, device_id_type=MESH,
        ).wait_recv()

        def rows_step(i, carry):
            rows = pl.ds(pl.multiple_of(i * rows_of, rows_of), rows_of)
            piece = (dot(source[rows, :], met[p]) * math.sqrt(2.0 / source.shape[1])).astype(jnp.bfloat16)
            planes[nb, c, rows, :] = piece
            each_way(nb, more_up, more_down, i, start)
            return carry

        lax.fori_loop(0, PIECES, rows_step, 0)

    def ways(i):
        up = pick([int(OWNER[row[i]] < at and at < chips - 1) for at, row in enumerate(ORDER)]) == 1
        down = pick([int(OWNER[row[i]] > at and at > 0) for at, row in enumerate(ORDER)]) == 1
        return up, down

    def passed_slice(i, nb):
        up, down = ways(i)

        def step(piece, carry):
            plane_copy(0, nb, c, piece).wait_recv()
            each_way(nb, up, down, piece, start)
            return carry

        lax.fori_loop(0, PIECES, step, 0)

    def columns(nb):
        return pl.ds(pl.multiple_of(nb * BLOCK, BLOCK), BLOCK)

    def half_slice(nb):
        whole_copy(2, pl.ds(nb, 1), twin_recv.at[nb]).wait_recv()
        sign = (1 - 2 * lax.rem(nb, 2)).astype(jnp.float32) * math.sqrt(2.0 / NSLOW)
        both = jnp.concatenate([planes[nb, 0], planes[nb, 1]], axis=1)
        part = (dot(mine[...], both) * sign).astype(jnp.bfloat16)
        half_way[:shots, columns(nb)] = part[:, :BLOCK]
        half_way[shots:, columns(nb)] = part[:, BLOCK:]

    def mix(both):
        real = both[:shots, :BLOCK] - both[shots:, BLOCK:]
        return real, both[:shots, BLOCK:] + both[shots:, :BLOCK]

    def back_new(nb):
        both = jnp.concatenate([planes[nb, 0], planes[nb, 1]], axis=1)
        return mix(dot(half_way[...], both))

    def back_more(nb, late):
        both = jnp.concatenate([planes[nb, 0, columns(late), :], planes[nb, 1, columns(late), :]], axis=1)
        real, imaginary = mix(dot(half_way[:, columns(late)], both))
        return total[nb, :shots] + real, total[nb, shots:] + imaginary

    def keep_total(nb, parts):
        total[nb, :shots] = parts[0]
        total[nb, shots:] = parts[1]

    def keep_back(nb, parts):
        back[:shots, columns(nb)] = (parts[0] * math.sqrt(1.0 / NSLOW)).astype(jnp.bfloat16)
        back[shots:, columns(nb)] = (parts[1] * math.sqrt(1.0 / NSLOW)).astype(jnp.bfloat16)

    def add_late(n, keep, unroll):
        late = nth(n)

        def step(i, carry):
            keep(nth(i), back_more(nth(i), late))
            return carry

        if n > 0:
            lax.fori_loop(0, n, step, 0, unroll=unroll)
        keep(late, back_new(late))

    for i in range(BLOCKS):
        nb = nth(i)
        owners = [row[i] in own for row, own in zip(ORDER, OWN)]
        mine_now = pick([int(x) for x in owners]) == 1
        if any(owners):
            @pl.when(mine_now)
            def _():
                own_slice(nb)
        if not all(owners):
            @pl.when(jnp.logical_not(mine_now))
            def _():
                passed_slice(i, nb)
        if 0 < i < BLOCKS - 1:
            half_slice(nth(i - 1))
            add_late(i - 1, keep_total, 1)
        if i == BLOCKS - 2:
            half_slice(nb)
            add_late(i, keep_total, 1)

    sent = outgoing.at[pl.ds(0, 2 * BLOCKS - len(OWN[0]))]
    pltpu.make_async_remote_copy(
        src_ref=sent, dst_ref=sent, send_sem=spread_send, recv_sem=spread_recv.at[0],
        device_id={"rep": 1 - c}, device_id_type=MESH,
    ).wait_send()
    half_slice(nth(BLOCKS - 1))
    add_late(BLOCKS - 1, keep_back, True)
    for at in range(chips):
        counts = [sum(owner <= at for owner in OWNER), sum(owner >= at for owner in OWNER)]

        @pl.when(z == at)
        def _():
            for way, count in enumerate(counts):
                if count < BLOCKS:
                    whole_copy(way, pl.ds(0, count), twin_recv.at[0]).wait_send()

    whole_copy(2, pl.ds(0, BLOCKS), twin_recv.at[0]).wait_send()


def one_frequency_fused(first_hertz, data, receiver_x, source_x):
    shots, rec_count = data.shape[1:]
    src_count = source_x.shape[0]
    group = 2 * len(OWN)
    vmem = pl.BlockSpec(memory_space=pltpu.VMEM)
    half = jnp.bfloat16
    back, receiver = pl.pallas_call(
        functools.partial(whole_kernel, first_hertz),
        out_shape=(
            jax.ShapeDtypeStruct((2 * shots, NSLOW), half),
            jax.ShapeDtypeStruct((NSLOW, rec_count), half),
        ),
        in_specs=[pl.BlockSpec(memory_space=pltpu.HBM)] * 3,
        out_specs=(vmem, vmem),
        scratch_shapes=[
            pltpu.VMEM((2 * shots, rec_count), half),
            pltpu.VMEM((1, rec_count), jnp.float32),
            pltpu.VMEM((1, src_count), jnp.float32),
            pltpu.VMEM((NSLOW, src_count), half),
            pltpu.VMEM((2, COARSE + FINE, rec_count), jnp.float32),
            pltpu.VMEM((2, COARSE + FINE, src_count), jnp.float32),
            pltpu.VMEM((shots, NSLOW), half),
            pltpu.VMEM((2 * BLOCKS, shots, BLOCK), half),
            pltpu.VMEM((PAIRS, src_count, BLOCK), half),
            pltpu.VMEM((BLOCKS, 2, NSLOW, BLOCK), half),
            pltpu.VMEM((2 * shots, NSLOW), half),
            pltpu.VMEM((BLOCKS, 2 * shots, BLOCK), jnp.float32),
            pltpu.SemaphoreType.DMA,
            pltpu.SemaphoreType.DMA((PAIRS,)),
            pltpu.SemaphoreType.DMA((3,)),
            pltpu.SemaphoreType.DMA((BLOCKS, PIECES)),
            pltpu.SemaphoreType.DMA((BLOCKS,)),
            pltpu.SemaphoreType.DMA((3,)),
        ],
        compiler_params=pltpu.CompilerParams(
            collective_id=0, has_side_effects=True, vmem_limit_bytes=30 * 1024 * 1024
        ),
        name="plane_wave_multiples",
    )(*[
        pltpu.with_memory_space_constraint(x, pltpu.HBM)
        for x in (data.reshape(2 * shots, rec_count), receiver_x.reshape(1, rec_count), source_x.reshape(1, src_count))
    ])
    result = (dot(back, receiver) * math.sqrt(2.0 / NSLOW)).astype(half)
    return result.reshape(2, shots, rec_count)


def fits(mesh_shape, shots):
    line = mesh_shape["shot"] == len(OWN) and mesh_shape["rep"] == 2
    return line and NSLOW == BLOCKS * BLOCK and shots % 128 == 0


def body(fused, recorded, receiver_x, source_x):
    per_device = recorded.shape[1]
    first_freq = lax.axis_index("freq") * per_device
    outs = []
    for k in range(per_device):
        omega = two_pi * (base_hertz + step_hertz * (first_freq + k).astype(jnp.float32))
        if fused(recorded.shape[2]):
            first_hertz = functools.partial(lambda k, f: f * per_device + k, k)
            outs.append(one_frequency_fused(first_hertz, recorded[:, k], receiver_x, source_x))
        else:
            outs.append(one_frequency(recorded[:, k], receiver_x, source_x, omega))
    return jnp.stack(outs, axis=1)


def solution(mesh):
    return jax.shard_map(
        functools.partial(body, functools.partial(fits, mesh.shape)),
        mesh=mesh,
        in_specs=(P(None, ("parts", "freq"), ("shot", "rep"), None), P("parts"), P("parts")),
        out_specs=P(None, ("parts", "freq"), ("shot", "rep"), None),
        check_vma=False,
    )
```

```python
import functools
import math

import jax
import jax.numpy as jnp
from jax import lax
from jax.experimental import pallas as pl
from jax.experimental.pallas import tpu as pltpu
from jax.sharding import PartitionSpec as P

NSLOW = 1024

two_pi = 6.283185307179586
base_hertz = 40.0
step_hertz = 0.5
slow_max = 0.0005
GROUP = ("shot", "rep")


def angle_table(omega, positions):
    half = NSLOW // 2
    fine = math.gcd(half, 16)
    unit = (omega * (slow_max / NSLOW)) * positions
    coarse = (jnp.arange(half // fine, dtype=jnp.int32) * (2 * fine)).astype(jnp.float32)[:, None] * unit
    small = (2 * jnp.arange(fine, dtype=jnp.int32) + 1).astype(jnp.float32)[:, None] * unit
    cos_a, sin_a = jnp.cos(coarse)[:, None], jnp.sin(coarse)[:, None]
    cos_b, sin_b = jnp.cos(small)[None], jnp.sin(small)[None]
    cosine = cos_a * cos_b - sin_a * sin_b
    sine = sin_a * cos_b + cos_a * sin_b
    return jnp.stack([cosine, sine]).astype(jnp.bfloat16).reshape(NSLOW, positions.shape[0])


def product(form, left, right):
    return jnp.einsum(form, left, right, preferred_element_type=jnp.float32)


def one_frequency(data, receiver_x, source_x, omega):
    shots = data.shape[1]
    src_count, rec_count = source_x.shape[0], receiver_x.shape[0]
    receiver = angle_table(omega, receiver_x)
    source = angle_table(omega, source_x)
    first = lax.axis_index(GROUP) * shots
    mine = angle_table(omega, lax.dynamic_slice_in_dim(source_x, first, shots, 0))
    spread = (product("csr,jr->csj", data, receiver) * math.sqrt(2.0 / rec_count)).astype(jnp.bfloat16)
    met = lax.all_to_all(spread, GROUP, split_axis=2, concat_axis=1, tiled=True)
    plane = (product("qs,csj->cqj", source, met) * math.sqrt(2.0 / src_count)).astype(jnp.bfloat16)
    planes = lax.all_gather(plane, GROUP, axis=2, tiled=True)
    sign = jnp.where(jnp.arange(NSLOW) < NSLOW // 2, 1.0, -1.0) * math.sqrt(2.0 / NSLOW)
    half_way = (product("qs,cqj->csj", mine, planes) * sign).astype(jnp.bfloat16)
    back_real = product("sm,mj->sj", half_way[0], planes[0]) - product("sm,mj->sj", half_way[1], planes[1])
    back_imaginary = product("sm,mj->sj", half_way[0], planes[1]) + product("sm,mj->sj", half_way[1], planes[0])
    back = (jnp.stack([back_real, back_imaginary]) * math.sqrt(1.0 / NSLOW)).astype(jnp.bfloat16)
    return (product("csj,jr->csr", back, receiver) * math.sqrt(2.0 / NSLOW)).astype(jnp.bfloat16)


FINE = 16
HALF = NSLOW // 2
COARSE = HALF // FINE
BLOCK = 128
PAIRS = HALF // BLOCK
PIECES = 4
MESH = pl.DeviceIdType.MESH

OWNER = tuple(2 * s + p % 2 for p in range(PAIRS) for s in range(2))
OWN = tuple(tuple(nb for nb, owner in enumerate(OWNER) if owner == at) for at in range(4))
ORDER = (
    (0, 2, 4, 6, 1, 5, 3, 7),
    (2, 6, 1, 0, 5, 4, 3, 7),
    (1, 5, 2, 3, 6, 7, 0, 4),
    (3, 1, 7, 5, 2, 6, 0, 4),
)
BLOCKS = len(OWNER)


def fill_factors(omega, positions, factors, fine, first, rows):
    count = positions.shape[1]
    tile = math.gcd(count, 256)
    sines = [(-1.0) ** n / math.factorial(2 * n + 1) for n in range(7)]
    cosines = [(-1.0) ** n / math.factorial(2 * n) for n in range(8)]
    turn_high = 6.28125
    turn_low = two_pi - turn_high

    def step(i, carry):
        lanes = pl.ds(pl.multiple_of(i * tile, tile), tile)
        unit = positions[:, lanes] * (omega * (slow_max / NSLOW))
        row = lax.broadcasted_iota(jnp.int32, (fine + rows, tile), 0)
        steps = jnp.where(row < fine, 2 * row + 1, (row - fine + first) * (2 * FINE)).astype(jnp.float32)
        phase = steps * unit
        turns = jnp.floor(phase * (1.0 / two_pi) + 0.5)
        half = 0.5 * ((phase - turns * turn_high) - turns * turn_low)
        square = half * half
        sine, cosine = sines[-1], cosines[-1]
        for term in reversed(sines[:-1]):
            sine = sine * square + term
        for term in reversed(cosines[:-1]):
            cosine = cosine * square + term
        sine = sine * half
        for i, values in enumerate((1.0 - 2.0 * sine * sine, 2.0 * sine * cosine)):
            if fine:
                factors[i, :fine, lanes] = values[:fine]
            factors[i, pl.ds(FINE + first, rows), lanes] = values[fine:]
        return carry

    lax.fori_loop(0, count // tile, step, 0)


def fill_pair(factors, table, p):
    count = table.shape[1]
    tile = math.gcd(count, 512)
    steps = BLOCK // FINE
    for first in range(0, count, tile):
        lanes = slice(first, first + tile)
        cos_b = factors[0, :FINE, lanes]
        sin_b = factors[1, :FINE, lanes]

        def step(a, carry):
            cos_a = factors[0, pl.ds(FINE + p * steps + a, 1), lanes]
            sin_a = factors[1, pl.ds(FINE + p * steps + a, 1), lanes]
            row = pl.multiple_of(2 * BLOCK * p + a * FINE, FINE)
            table[pl.ds(row, FINE), lanes] = (cos_a * cos_b - sin_a * sin_b).astype(jnp.bfloat16)
            table[pl.ds(row + BLOCK, FINE), lanes] = (sin_a * cos_b + cos_a * sin_b).astype(jnp.bfloat16)
            return carry

        lax.fori_loop(0, steps, step, 0, unroll=4)


def dot(left, right):
    return jnp.dot(left, right, preferred_element_type=jnp.float32)


def whole_kernel(
    first_hertz, data_in, receiver_in, source_in, back, receiver,
    data, receiver_x, source_x, source, receiver_f, source_f, mine, outgoing, met, planes, half_way, total,
    spread_send, spread_recv, plane_send, plane_recv, twin_recv, load_sem,
):
    chips, cores = len(OWN), 2
    coarse = BLOCK // FINE
    group = chips * cores
    shots = data.shape[0] // 2
    z, c = lax.axis_index("shot"), lax.axis_index("rep")
    me = z * cores + c
    side = z // 2
    more_up, more_down = z < chips - 1, z > 0

    def pick(values):
        out = jnp.int32(values[-1])
        for i, value in enumerate(values[:-1]):
            out = jnp.where(z == i, jnp.int32(value), out)
        return out

    packed = pick([sum(nb << (3 * i) for i, nb in enumerate(row)) for row in ORDER])

    def nth(i):
        return lax.rem(packed >> (3 * i), BLOCKS)

    def place(d):
        return {"shot": d // cores, "rep": d % cores}

    loads = [
        pltpu.make_async_copy(src, dst, load_sem.at[i])
        for i, (src, dst) in enumerate(((receiver_in, receiver_x), (data_in, data), (source_in, source_x)))
    ]
    for load in loads:
        load.start()
    barrier = pltpu.get_barrier_semaphore()
    for d in range(group):
        @pl.when(d != me)
        def _():
            pl.semaphore_signal(barrier, inc=1, device_id=place(d), device_id_type=MESH)

    hertz = first_hertz(lax.axis_index("freq")).astype(jnp.float32)
    omega = two_pi * (base_hertz + step_hertz * hertz)
    own_rows = pl.ds(pl.multiple_of(me * shots, shots), shots)

    def spread_copy(p, s, h, to):
        return pltpu.make_async_remote_copy(
            src_ref=outgoing.at[4 * p + 2 * s + h], dst_ref=met.at[p, own_rows],
            send_sem=spread_send, recv_sem=spread_recv.at[p],
            device_id={"shot": to, "rep": h}, device_id_type=MESH,
        )

    def put(p, h, part):
        part = (part * math.sqrt(2.0 / data.shape[1])).astype(jnp.bfloat16)
        for s in range(2):
            piece = part[:, s * BLOCK : (s + 1) * BLOCK]
            here = me == (2 * s + lax.rem(p, 2)) * cores + h

            @pl.when(here)
            def _():
                met[p, own_rows, :] = piece

            @pl.when(jnp.logical_not(here))
            def _():
                outgoing[4 * p + 2 * s + h] = piece

    def send(p, h):
        for k in range(2):
            s = lax.rem(1 - side + c + k, 2)
            to = 2 * s + lax.rem(p, 2)

            @pl.when((to != z) | (c != h))
            def _():
                spread_copy(p, s, h, to).start()

    def spread(p, rows):
        return lax.dot_general(
            data[rows, :], receiver[pl.ds(pl.multiple_of(2 * BLOCK * p, 2 * BLOCK), 2 * BLOCK), :], (((1,), (1,)), ((), ())),
            preferred_element_type=jnp.float32,
        )

    loads[0].wait()
    fill_factors(omega, receiver_x, receiver_f, FINE, side * coarse, coarse)
    fill_pair(receiver_f, receiver, side)
    loads[1].wait()
    for h in range(2):
        put(side, h, spread(side, slice(h * shots, (h + 1) * shots)))
        if h == 0:
            pl.semaphore_wait(barrier, group - 1)
        send(side, h)
    fill_factors(omega, receiver_x, receiver_f, 0, 0, COARSE)
    for j in range(1, PAIRS):
        p = j - side if j % 2 else j + side
        fill_pair(receiver_f, receiver, p)
        part = spread(p, slice(0, 2 * shots))
        for h in range(2):
            put(p, h, part[h * shots : (h + 1) * shots])
        for h in range(2):
            send(p, h)

    loads[2].wait()
    fill_factors(omega, source_x, source_f, FINE, 0, COARSE)
    for p in range(PAIRS):
        fill_pair(source_f, source, p)
    mine[...] = source[:, own_rows].T
    half_way[...] = jnp.zeros_like(half_way)

    rows_of = NSLOW // PIECES

    def plane_copy(way, nb, h, piece):
        to = [{"shot": z + 1, "rep": c}, {"shot": z - 1, "rep": c}, {"shot": z, "rep": 1 - c}][way]
        part = planes.at[nb, h, pl.ds(pl.multiple_of(piece * rows_of, rows_of), rows_of)]
        return pltpu.make_async_remote_copy(
            src_ref=part, dst_ref=part, send_sem=plane_send.at[way],
            recv_sem=twin_recv.at[nb] if way == 2 else plane_recv.at[nb, piece],
            device_id=to, device_id_type=MESH,
        )

    def whole_copy(way, blocks, recv_sem):
        part = planes.at[blocks, 0]
        return pltpu.make_async_remote_copy(
            src_ref=part, dst_ref=part, send_sem=plane_send.at[way], recv_sem=recv_sem,
            device_id={"rep": 1 - c}, device_id_type=MESH,
        )

    def each_way(nb, up, down, piece, act):
        @pl.when(up)
        def _():
            act(plane_copy(0, nb, c, piece))

        @pl.when(down)
        def _():
            act(plane_copy(1, nb, c, piece))

        act(plane_copy(2, nb, c, piece))

    def start(copy):
        copy.start()

    def own_slice(nb):
        p = nb // 2
        arrived = met.at[p, pl.ds(0, (group - 1) * shots)]
        pltpu.make_async_remote_copy(
            src_ref=arrived, dst_ref=arrived, send_sem=spread_send, recv_sem=spread_recv.at[p],
            device_id={"rep": 1 - c}, device_id_type=MESH,
        ).wait_recv()

        def rows_step(i, carry):
            rows = pl.ds(pl.multiple_of(i * rows_of, rows_of), rows_of)
            piece = (dot(source[rows, :], met[p]) * math.sqrt(2.0 / source.shape[1])).astype(jnp.bfloat16)
            planes[nb, c, rows, :] = piece
            each_way(nb, more_up, more_down, i, start)
            return carry

        lax.fori_loop(0, PIECES, rows_step, 0)

    def ways(i):
        up = pick([int(OWNER[row[i]] < at and at < chips - 1) for at, row in enumerate(ORDER)]) == 1
        down = pick([int(OWNER[row[i]] > at and at > 0) for at, row in enumerate(ORDER)]) == 1
        return up, down

    def passed_slice(i, nb):
        up, down = ways(i)

        def step(piece, carry):
            plane_copy(0, nb, c, piece).wait_recv()
            each_way(nb, up, down, piece, start)
            return carry

        lax.fori_loop(0, PIECES, step, 0)

    def columns(nb):
        return pl.ds(pl.multiple_of(nb * BLOCK, BLOCK), BLOCK)

    def half_slice(nb):
        whole_copy(2, pl.ds(nb, 1), twin_recv.at[nb]).wait_recv()
        sign = (1 - 2 * lax.rem(nb, 2)).astype(jnp.float32) * math.sqrt(2.0 / NSLOW)
        both = jnp.concatenate([planes[nb, 0], planes[nb, 1]], axis=1)
        part = (dot(mine[...], both) * sign).astype(jnp.bfloat16)
        half_way[:shots, columns(nb)] = part[:, :BLOCK]
        half_way[shots:, columns(nb)] = part[:, BLOCK:]

    def mix(both):
        real = both[:shots, :BLOCK] - both[shots:, BLOCK:]
        return real, both[:shots, BLOCK:] + both[shots:, :BLOCK]

    def back_new(nb):
        both = jnp.concatenate([planes[nb, 0], planes[nb, 1]], axis=1)
        return mix(dot(half_way[...], both))

    def back_more(nb, late):
        both = jnp.concatenate([planes[nb, 0, columns(late), :], planes[nb, 1, columns(late), :]], axis=1)
        real, imaginary = mix(dot(half_way[:, columns(late)], both))
        return total[nb, :shots] + real, total[nb, shots:] + imaginary

    def keep_total(nb, parts):
        total[nb, :shots] = parts[0]
        total[nb, shots:] = parts[1]

    def keep_back(nb, parts):
        back[:shots, columns(nb)] = (parts[0] * math.sqrt(1.0 / NSLOW)).astype(jnp.bfloat16)
        back[shots:, columns(nb)] = (parts[1] * math.sqrt(1.0 / NSLOW)).astype(jnp.bfloat16)

    def add_late(n, keep, unroll):
        late = nth(n)

        def step(i, carry):
            keep(nth(i), back_more(nth(i), late))
            return carry

        if n > 0:
            lax.fori_loop(0, n, step, 0, unroll=unroll)
        keep(late, back_new(late))

    for i in range(BLOCKS):
        nb = nth(i)
        owners = [row[i] in own for row, own in zip(ORDER, OWN)]
        mine_now = pick([int(x) for x in owners]) == 1
        if any(owners):
            @pl.when(mine_now)
            def _():
                own_slice(nb)
        if not all(owners):
            @pl.when(jnp.logical_not(mine_now))
            def _():
                passed_slice(i, nb)
        if 0 < i < BLOCKS - 1:
            half_slice(nth(i - 1))
            add_late(i - 1, keep_total, 1)
        if i == BLOCKS - 2:
            half_slice(nb)
            add_late(i, keep_total, 1)

    sent = outgoing.at[pl.ds(0, 2 * BLOCKS - len(OWN[0]))]
    pltpu.make_async_remote_copy(
        src_ref=sent, dst_ref=sent, send_sem=spread_send, recv_sem=spread_recv.at[0],
        device_id={"rep": 1 - c}, device_id_type=MESH,
    ).wait_send()
    half_slice(nth(BLOCKS - 1))
    add_late(BLOCKS - 1, keep_back, True)
    for at in range(chips):
        counts = [sum(owner <= at for owner in OWNER), sum(owner >= at for owner in OWNER)]

        @pl.when(z == at)
        def _():
            for way, count in enumerate(counts):
                if count < BLOCKS:
                    whole_copy(way, pl.ds(0, count), twin_recv.at[0]).wait_send()

    whole_copy(2, pl.ds(0, BLOCKS), twin_recv.at[0]).wait_send()


def one_frequency_fused(first_hertz, data, receiver_x, source_x):
    shots, rec_count = data.shape[1:]
    src_count = source_x.shape[0]
    group = 2 * len(OWN)
    vmem = pl.BlockSpec(memory_space=pltpu.VMEM)
    half = jnp.bfloat16
    back, receiver = pl.pallas_call(
        functools.partial(whole_kernel, first_hertz),
        out_shape=(
            jax.ShapeDtypeStruct((2 * shots, NSLOW), half),
            jax.ShapeDtypeStruct((NSLOW, rec_count), half),
        ),
        in_specs=[pl.BlockSpec(memory_space=pltpu.HBM)] * 3,
        out_specs=(vmem, vmem),
        scratch_shapes=[
            pltpu.VMEM((2 * shots, rec_count), half),
            pltpu.VMEM((1, rec_count), jnp.float32),
            pltpu.VMEM((1, src_count), jnp.float32),
            pltpu.VMEM((NSLOW, src_count), half),
            pltpu.VMEM((2, COARSE + FINE, rec_count), jnp.float32),
            pltpu.VMEM((2, COARSE + FINE, src_count), jnp.float32),
            pltpu.VMEM((shots, NSLOW), half),
            pltpu.VMEM((2 * BLOCKS, shots, BLOCK), half),
            pltpu.VMEM((PAIRS, src_count, BLOCK), half),
            pltpu.VMEM((BLOCKS, 2, NSLOW, BLOCK), half),
            pltpu.VMEM((2 * shots, NSLOW), half),
            pltpu.VMEM((BLOCKS, 2 * shots, BLOCK), jnp.float32),
            pltpu.SemaphoreType.DMA,
            pltpu.SemaphoreType.DMA((PAIRS,)),
            pltpu.SemaphoreType.DMA((3,)),
            pltpu.SemaphoreType.DMA((BLOCKS, PIECES)),
            pltpu.SemaphoreType.DMA((BLOCKS,)),
            pltpu.SemaphoreType.DMA((3,)),
        ],
        compiler_params=pltpu.CompilerParams(
            collective_id=0, has_side_effects=True, vmem_limit_bytes=30 * 1024 * 1024
        ),
        name="plane_wave_multiples",
    )(*[
        pltpu.with_memory_space_constraint(x, pltpu.HBM)
        for x in (data.reshape(2 * shots, rec_count), receiver_x.reshape(1, rec_count), source_x.reshape(1, src_count))
    ])
    result = (dot(back, receiver) * math.sqrt(2.0 / NSLOW)).astype(half)
    return result.reshape(2, shots, rec_count)


def fits(mesh_shape, shots):
    line = mesh_shape["shot"] == len(OWN) and mesh_shape["rep"] == 2
    return line and NSLOW == BLOCKS * BLOCK and shots % 128 == 0


def body(fused, recorded, receiver_x, source_x):
    per_device = recorded.shape[1]
    first_freq = lax.axis_index("freq") * per_device
    outs = []
    for k in range(per_device):
        omega = two_pi * (base_hertz + step_hertz * (first_freq + k).astype(jnp.float32))
        if fused(recorded.shape[2]):
            first_hertz = functools.partial(lambda k, f: f * per_device + k, k)
            outs.append(one_frequency_fused(first_hertz, recorded[:, k], receiver_x, source_x))
        else:
            outs.append(one_frequency(recorded[:, k], receiver_x, source_x, omega))
    return jnp.stack(outs, axis=1)


def solution(mesh):
    return jax.shard_map(
        functools.partial(body, functools.partial(fits, mesh.shape)),
        mesh=mesh,
        in_specs=(P(None, ("parts", "freq"), ("shot", "rep"), None), P("parts"), P("parts")),
        out_specs=P(None, ("parts", "freq"), ("shot", "rep"), None),
        check_vma=False,
    )
```

```python
import functools
import math

import jax
import jax.numpy as jnp
from jax import lax
from jax.experimental import pallas as pl
from jax.experimental.pallas import tpu as pltpu
from jax.sharding import PartitionSpec as P

NSLOW = 1024

two_pi = 6.283185307179586
base_hertz = 40.0
step_hertz = 0.5
slow_max = 0.0005
GROUP = ("shot", "rep")


def angle_table(omega, positions):
    half = NSLOW // 2
    fine = math.gcd(half, 16)
    unit = (omega * (slow_max / NSLOW)) * positions
    coarse = (jnp.arange(half // fine, dtype=jnp.int32) * (2 * fine)).astype(jnp.float32)[:, None] * unit
    small = (2 * jnp.arange(fine, dtype=jnp.int32) + 1).astype(jnp.float32)[:, None] * unit
    cos_a, sin_a = jnp.cos(coarse)[:, None], jnp.sin(coarse)[:, None]
    cos_b, sin_b = jnp.cos(small)[None], jnp.sin(small)[None]
    cosine = cos_a * cos_b - sin_a * sin_b
    sine = sin_a * cos_b + cos_a * sin_b
    return jnp.stack([cosine, sine]).astype(jnp.bfloat16).reshape(NSLOW, positions.shape[0])


def product(form, left, right):
    return jnp.einsum(form, left, right, preferred_element_type=jnp.float32)


def one_frequency(data, receiver_x, source_x, omega):
    shots = data.shape[1]
    src_count, rec_count = source_x.shape[0], receiver_x.shape[0]
    receiver = angle_table(omega, receiver_x)
    source = angle_table(omega, source_x)
    first = lax.axis_index(GROUP) * shots
    mine = angle_table(omega, lax.dynamic_slice_in_dim(source_x, first, shots, 0))
    spread = (product("csr,jr->csj", data, receiver) * math.sqrt(2.0 / rec_count)).astype(jnp.bfloat16)
    met = lax.all_to_all(spread, GROUP, split_axis=2, concat_axis=1, tiled=True)
    plane = (product("qs,csj->cqj", source, met) * math.sqrt(2.0 / src_count)).astype(jnp.bfloat16)
    planes = lax.all_gather(plane, GROUP, axis=2, tiled=True)
    sign = jnp.where(jnp.arange(NSLOW) < NSLOW // 2, 1.0, -1.0) * math.sqrt(2.0 / NSLOW)
    half_way = (product("qs,cqj->csj", mine, planes) * sign).astype(jnp.bfloat16)
    back_real = product("sm,mj->sj", half_way[0], planes[0]) - product("sm,mj->sj", half_way[1], planes[1])
    back_imaginary = product("sm,mj->sj", half_way[0], planes[1]) + product("sm,mj->sj", half_way[1], planes[0])
    back = (jnp.stack([back_real, back_imaginary]) * math.sqrt(1.0 / NSLOW)).astype(jnp.bfloat16)
    return (product("csj,jr->csr", back, receiver) * math.sqrt(2.0 / NSLOW)).astype(jnp.bfloat16)


FINE = 16
HALF = NSLOW // 2
COARSE = HALF // FINE
BLOCK = 128
PAIRS = HALF // BLOCK
PIECES = 4
MESH = pl.DeviceIdType.MESH

OWNER = tuple(2 * s + p % 2 for p in range(PAIRS) for s in range(2))
OWN = tuple(tuple(nb for nb, owner in enumerate(OWNER) if owner == at) for at in range(4))
ORDER = (
    (0, 2, 4, 6, 1, 5, 3, 7),
    (2, 6, 1, 0, 5, 4, 3, 7),
    (1, 5, 2, 3, 6, 7, 0, 4),
    (3, 1, 7, 5, 2, 6, 0, 4),
)
SENDING = (
    (0, 1, 2, 3, 4, 5, 6, 7),
    (0, 1, 4, 3, 5, 7, 2, 6),
    (2, 3, 0, 7, 6, 4, 1, 5),
    (2, 3, 0, 1, 6, 7, 4, 5),
)
BLOCKS = len(OWNER)


def fill_factors(omega, positions, factors, fine, first, rows):
    count = positions.shape[1]
    tile = math.gcd(count, 256)
    sines = [(-1.0) ** n / math.factorial(2 * n + 1) for n in range(7)]
    cosines = [(-1.0) ** n / math.factorial(2 * n) for n in range(8)]
    turn_high = 6.28125
    turn_low = two_pi - turn_high

    def step(i, carry):
        lanes = pl.ds(pl.multiple_of(i * tile, tile), tile)
        unit = positions[:, lanes] * (omega * (slow_max / NSLOW))
        row = lax.broadcasted_iota(jnp.int32, (fine + rows, tile), 0)
        steps = jnp.where(row < fine, 2 * row + 1, (row - fine + first) * (2 * FINE)).astype(jnp.float32)
        phase = steps * unit
        turns = jnp.floor(phase * (1.0 / two_pi) + 0.5)
        half = 0.5 * ((phase - turns * turn_high) - turns * turn_low)
        square = half * half
        sine, cosine = sines[-1], cosines[-1]
        for term in reversed(sines[:-1]):
            sine = sine * square + term
        for term in reversed(cosines[:-1]):
            cosine = cosine * square + term
        sine = sine * half
        for i, values in enumerate((1.0 - 2.0 * sine * sine, 2.0 * sine * cosine)):
            if fine:
                factors[i, :fine, lanes] = values[:fine]
            factors[i, pl.ds(FINE + first, rows), lanes] = values[fine:]
        return carry

    lax.fori_loop(0, count // tile, step, 0)


def fill_pair(factors, table, p):
    count = table.shape[1]
    tile = math.gcd(count, 512)
    steps = BLOCK // FINE
    for first in range(0, count, tile):
        lanes = slice(first, first + tile)
        cos_b = factors[0, :FINE, lanes]
        sin_b = factors[1, :FINE, lanes]

        def step(a, carry):
            cos_a = factors[0, pl.ds(FINE + p * steps + a, 1), lanes]
            sin_a = factors[1, pl.ds(FINE + p * steps + a, 1), lanes]
            row = pl.multiple_of(2 * BLOCK * p + a * FINE, FINE)
            table[pl.ds(row, FINE), lanes] = (cos_a * cos_b - sin_a * sin_b).astype(jnp.bfloat16)
            table[pl.ds(row + BLOCK, FINE), lanes] = (sin_a * cos_b + cos_a * sin_b).astype(jnp.bfloat16)
            return carry

        lax.fori_loop(0, steps, step, 0, unroll=4)


def dot(left, right):
    return jnp.dot(left, right, preferred_element_type=jnp.float32)


def whole_kernel(
    first_hertz, data_in, receiver_in, source_in, result, last_left, last_right,
    data, receiver_x, source_x, receiver, source, receiver_f, source_f, mine, outgoing, met, planes, half_way,
    total, back, crossed,
    spread_send, spread_recv, plane_send, plane_recv, twin_recv, load_sem,
):
    chips, cores = len(OWN), 2
    coarse = BLOCK // FINE
    group = chips * cores
    shots = data.shape[0] // 2
    z, c = lax.axis_index("shot"), lax.axis_index("rep")
    me = z * cores + c
    side = z // 2
    more_up, more_down = z < chips - 1, z > 0

    def pick(values):
        out = jnp.int32(values[-1])
        for i, value in enumerate(values[:-1]):
            out = jnp.where(z == i, jnp.int32(value), out)
        return out

    packed = pick([sum(nb << (3 * i) for i, nb in enumerate(row)) for row in ORDER])
    sending = pick([sum(nb << (3 * i) for i, nb in enumerate(row)) for row in SENDING])

    def nth(i):
        return lax.rem(packed >> (3 * i), BLOCKS)

    def owner_of(nb):
        return 2 * lax.rem(nb, 2) + lax.rem(nb // 2, 2)

    def block_rows(nb):
        return pl.ds(pl.multiple_of(nb * BLOCK, BLOCK), BLOCK)

    def place(d):
        return {"shot": d // cores, "rep": d % cores}

    loads = [
        pltpu.make_async_copy(src, dst, load_sem.at[i])
        for i, (src, dst) in enumerate(((receiver_in, receiver_x), (data_in, data), (source_in, source_x)))
    ]
    for load in loads:
        load.start()
    barrier = pltpu.get_barrier_semaphore()
    for d in range(group):
        @pl.when(d != me)
        def _():
            pl.semaphore_signal(barrier, inc=1, device_id=place(d), device_id_type=MESH)

    hertz = first_hertz(lax.axis_index("freq")).astype(jnp.float32)
    omega = two_pi * (base_hertz + step_hertz * hertz)
    own_rows = pl.ds(pl.multiple_of(me * shots, shots), shots)

    def put(blocks, h, part):
        part = (part * math.sqrt(2.0 / data.shape[1])).astype(jnp.bfloat16)
        for s, nb in enumerate(blocks):
            piece = part[:, s * BLOCK : (s + 1) * BLOCK]
            here = me == owner_of(nb) * cores + h

            @pl.when(here)
            def _():
                met[nb // 2, own_rows, :] = piece

            @pl.when(jnp.logical_not(here))
            def _():
                outgoing[2 * nb + h] = piece

    def send(blocks, h):
        for k in range(2):
            nb = jnp.where(lax.rem(1 - side + c + k, 2) == 0, *blocks)
            to = owner_of(nb)

            @pl.when((to != z) | (c != h))
            def _():
                pltpu.make_async_remote_copy(
                    src_ref=outgoing.at[2 * nb + h], dst_ref=met.at[nb // 2, own_rows],
                    send_sem=spread_send, recv_sem=spread_recv.at[nb // 2],
                    device_id={"shot": to, "rep": h}, device_id_type=MESH,
                ).start()

    def spread(blocks, rows):
        right = jnp.concatenate([receiver[block_rows(nb), :] for nb in blocks], axis=0)
        return lax.dot_general(data[rows, :], right, (((1,), (1,)), ((), ())), preferred_element_type=jnp.float32)

    loads[0].wait()
    fill_factors(omega, receiver_x, receiver_f, FINE, side * coarse, coarse)
    fill_pair(receiver_f, receiver, side)
    loads[1].wait()
    for step in range(PAIRS):
        blocks = [lax.rem(sending >> (3 * i), BLOCKS) for i in (2 * step, 2 * step + 1)]
        if step == 0:
            for h in range(2):
                put(blocks, h, spread(blocks, slice(h * shots, (h + 1) * shots)))
                if h == 0:
                    pl.semaphore_wait(barrier, group - 1)
                send(blocks, h)
            fill_factors(omega, receiver_x, receiver_f, 0, 0, COARSE)
            fill_pair(receiver_f, receiver, 1 - side)
            fill_pair(receiver_f, receiver, 2 + side)
            continue
        part = spread(blocks, slice(0, 2 * shots))
        for h in range(2):
            put(blocks, h, part[h * shots : (h + 1) * shots])
        for h in range(2):
            send(blocks, h)
        if step == 1:
            fill_pair(receiver_f, receiver, 3 - side)

    loads[2].wait()
    fill_factors(omega, source_x, source_f, FINE, 0, COARSE)
    for p in range(PAIRS):
        fill_pair(source_f, source, p)
    mine[...] = source[:, own_rows].T
    for ref in (half_way, back, crossed, last_left, last_right):
        ref[...] = jnp.zeros_like(ref)
    outer = (z == 0) | (z == chips - 1)

    rows_of = NSLOW // PIECES

    def plane_copy(way, nb, h, piece):
        to = [{"shot": z + 1, "rep": c}, {"shot": z - 1, "rep": c}, {"shot": z, "rep": 1 - c}][way]
        part = planes.at[nb, h, pl.ds(pl.multiple_of(piece * rows_of, rows_of), rows_of)]
        return pltpu.make_async_remote_copy(
            src_ref=part, dst_ref=part, send_sem=plane_send.at[way],
            recv_sem=twin_recv.at[nb] if way == 2 else plane_recv.at[nb, piece],
            device_id=to, device_id_type=MESH,
        )

    def whole_copy(way, blocks, recv_sem):
        part = planes.at[blocks, 0]
        return pltpu.make_async_remote_copy(
            src_ref=part, dst_ref=part, send_sem=plane_send.at[way], recv_sem=recv_sem,
            device_id={"rep": 1 - c}, device_id_type=MESH,
        )

    def each_way(nb, up, down, piece, act):
        @pl.when(up)
        def _():
            act(plane_copy(0, nb, c, piece))

        @pl.when(down)
        def _():
            act(plane_copy(1, nb, c, piece))

        act(plane_copy(2, nb, c, piece))

    def start(copy):
        copy.start()

    def own_slice(nb):
        p = nb // 2
        arrived = met.at[p, pl.ds(0, (group - 1) * shots)]
        pltpu.make_async_remote_copy(
            src_ref=arrived, dst_ref=arrived, send_sem=spread_send, recv_sem=spread_recv.at[p],
            device_id={"rep": 1 - c}, device_id_type=MESH,
        ).wait_recv()

        def rows_step(i, carry):
            rows = pl.ds(pl.multiple_of(i * rows_of, rows_of), rows_of)
            piece = (dot(source[rows, :], met[p]) * math.sqrt(2.0 / source.shape[1])).astype(jnp.bfloat16)
            planes[nb, c, rows, :] = piece
            each_way(nb, more_up, more_down, i, start)
            return carry

        lax.fori_loop(0, PIECES, rows_step, 0)

    def ways(i):
        up = pick([int(OWNER[row[i]] < at and at < chips - 1) for at, row in enumerate(ORDER)]) == 1
        down = pick([int(OWNER[row[i]] > at and at > 0) for at, row in enumerate(ORDER)]) == 1
        return up, down

    def passed_slice(i, nb):
        up, down = ways(i)

        def step(piece, carry):
            plane_copy(0, nb, c, piece).wait_recv()
            each_way(nb, up, down, piece, start)
            return carry

        lax.fori_loop(0, PIECES, step, 0)

    def columns(nb):
        return pl.ds(pl.multiple_of(nb * BLOCK, BLOCK), BLOCK)

    def half_slice(nb):
        whole_copy(2, pl.ds(nb, 1), twin_recv.at[nb]).wait_recv()
        sign = (1 - 2 * lax.rem(nb, 2)).astype(jnp.float32) * math.sqrt(2.0 / NSLOW)
        both = jnp.concatenate([planes[nb, 0], planes[nb, 1]], axis=1)
        part = (dot(mine[...], both) * sign).astype(jnp.bfloat16)
        half_way[:shots, columns(nb)] = part[:, :BLOCK]
        half_way[shots:, columns(nb)] = part[:, BLOCK:]

    def mix(both):
        real = both[:shots, :BLOCK] - both[shots:, BLOCK:]
        return real, both[:shots, BLOCK:] + both[shots:, :BLOCK]

    def back_new(nb):
        both = jnp.concatenate([planes[nb, 0], planes[nb, 1]], axis=1)
        return mix(dot(half_way[...], both))

    def back_more(nb, late):
        both = jnp.concatenate([planes[nb, 0, columns(late), :], planes[nb, 1, columns(late), :]], axis=1)
        real, imaginary = mix(dot(half_way[:, columns(late)], both))
        return total[nb, :shots] + real, total[nb, shots:] + imaginary

    def keep_total(nb, parts):
        total[nb, :shots] = parts[0]
        total[nb, shots:] = parts[1]

    def keep_back(nb, parts):
        back[:shots, columns(nb)] = (parts[0] * math.sqrt(1.0 / NSLOW)).astype(jnp.bfloat16)
        back[shots:, columns(nb)] = (parts[1] * math.sqrt(1.0 / NSLOW)).astype(jnp.bfloat16)

    def add_late(n, keep, keep_new):
        late = nth(n)
        for i in range(n):
            keep(nth(i), back_more(nth(i), late))
        keep_new(late, back_new(late))

    scale_back = math.sqrt(1.0 / NSLOW)
    rec_count = receiver.shape[1]
    tile = math.gcd(rec_count, 512)
    last, before = BLOCKS - 1, BLOCKS - 2

    def lanes_of(i):
        return pl.ds(pl.multiple_of(i * tile, tile), tile)

    def right_side():
        late = nth(last)
        for i in range(before):
            for h in range(2):
                crossed[h * BLOCK : (h + 1) * BLOCK, columns(nth(i))] = planes[nth(i), h, columns(late), :]
        last_right[2 * BLOCK : 3 * BLOCK, :] = receiver[columns(late), :]
        last_right[3 * BLOCK :, :] = receiver[columns(nth(before)), :]

        def step(i, carry):
            part = dot(crossed[...], receiver[:, lanes_of(i)])
            last_right[: 2 * BLOCK, lanes_of(i)] = (part * scale_back).astype(jnp.bfloat16)
            return carry

        lax.fori_loop(0, rec_count // tile, step, 0)

    def left_side():
        late = nth(last)
        half_slice(late)
        real, imaginary = half_way[:shots, columns(late)], half_way[shots:, columns(late)]
        last_left[:shots, :BLOCK] = real
        last_left[:shots, BLOCK : 2 * BLOCK] = -imaginary
        last_left[shots:, :BLOCK] = imaginary
        last_left[shots:, BLOCK : 2 * BLOCK] = real
        for at, parts in ((2, back_new(late)), (3, back_more(nth(before), late))):
            for rows, part in zip((slice(0, shots), slice(shots, 2 * shots)), parts):
                last_left[rows, at * BLOCK : (at + 1) * BLOCK] = (part * scale_back).astype(jnp.bfloat16)

    def result_so_far():
        def step(i, carry):
            result[:, lanes_of(i)] = dot(back[...], receiver[:, lanes_of(i)])
            return carry

        lax.fori_loop(0, rec_count // tile, step, 0)

    for i in range(BLOCKS):
        nb = nth(i)
        owners = [row[i] in own for row, own in zip(ORDER, OWN)]
        mine_now = pick([int(x) for x in owners]) == 1
        if any(owners):
            @pl.when(mine_now)
            def _():
                own_slice(nb)
        if not all(owners):
            @pl.when(jnp.logical_not(mine_now))
            def _():
                passed_slice(i, nb)
        if 0 < i < before:
            half_slice(nth(i - 1))
            add_late(i - 1, keep_total, keep_total)
        if i == before - 1:
            @pl.when(outer)
            def _():
                half_slice(nb)
                add_late(i, keep_total, keep_total)
                right_side()
        if i == before:
            @pl.when(jnp.logical_not(outer))
            def _():
                half_slice(nth(i - 1))
                add_late(i - 1, keep_total, keep_total)

            half_slice(nb)

            @pl.when(outer)
            def _():
                add_late(i, keep_back, keep_total)
                result_so_far()

            @pl.when(jnp.logical_not(outer))
            def _():
                add_late(i, keep_total, keep_total)

    sent = outgoing.at[pl.ds(0, 2 * BLOCKS - len(OWN[0]))]
    pltpu.make_async_remote_copy(
        src_ref=sent, dst_ref=sent, send_sem=spread_send, recv_sem=spread_recv.at[0],
        device_id={"rep": 1 - c}, device_id_type=MESH,
    ).wait_send()

    @pl.when(outer)
    def _():
        left_side()

    @pl.when(jnp.logical_not(outer))
    def _():
        half_slice(nth(last))
        add_late(last, keep_back, keep_back)
        result_so_far()

    for at in range(chips):
        counts = [sum(owner <= at for owner in OWNER), sum(owner >= at for owner in OWNER)]

        @pl.when(z == at)
        def _():
            for way, count in enumerate(counts):
                if count < BLOCKS:
                    whole_copy(way, pl.ds(0, count), twin_recv.at[0]).wait_send()

    whole_copy(2, pl.ds(0, BLOCKS), twin_recv.at[0]).wait_send()


def one_frequency_fused(first_hertz, data, receiver_x, source_x):
    shots, rec_count = data.shape[1:]
    src_count = source_x.shape[0]
    group = 2 * len(OWN)
    vmem = pl.BlockSpec(memory_space=pltpu.VMEM)
    half = jnp.bfloat16
    total, left, right = pl.pallas_call(
        functools.partial(whole_kernel, first_hertz),
        out_shape=(
            jax.ShapeDtypeStruct((2 * shots, rec_count), jnp.float32),
            jax.ShapeDtypeStruct((2 * shots, 4 * BLOCK), half),
            jax.ShapeDtypeStruct((4 * BLOCK, rec_count), half),
        ),
        in_specs=[pl.BlockSpec(memory_space=pltpu.HBM)] * 3,
        out_specs=(vmem, vmem, vmem),
        scratch_shapes=[
            pltpu.VMEM((2 * shots, rec_count), half),
            pltpu.VMEM((1, rec_count), jnp.float32),
            pltpu.VMEM((1, src_count), jnp.float32),
            pltpu.VMEM((NSLOW, rec_count), half),
            pltpu.VMEM((NSLOW, src_count), half),
            pltpu.VMEM((2, COARSE + FINE, rec_count), jnp.float32),
            pltpu.VMEM((2, COARSE + FINE, src_count), jnp.float32),
            pltpu.VMEM((shots, NSLOW), half),
            pltpu.VMEM((2 * BLOCKS, shots, BLOCK), half),
            pltpu.VMEM((PAIRS, src_count, BLOCK), half),
            pltpu.VMEM((BLOCKS, 2, NSLOW, BLOCK), half),
            pltpu.VMEM((2 * shots, NSLOW), half),
            pltpu.VMEM((BLOCKS, 2 * shots, BLOCK), jnp.float32),
            pltpu.VMEM((2 * shots, NSLOW), half),
            pltpu.VMEM((2 * BLOCK, NSLOW), half),
            pltpu.SemaphoreType.DMA,
            pltpu.SemaphoreType.DMA((PAIRS,)),
            pltpu.SemaphoreType.DMA((3,)),
            pltpu.SemaphoreType.DMA((BLOCKS, PIECES)),
            pltpu.SemaphoreType.DMA((BLOCKS,)),
            pltpu.SemaphoreType.DMA((3,)),
        ],
        compiler_params=pltpu.CompilerParams(
            collective_id=0, has_side_effects=True, vmem_limit_bytes=30 * 1024 * 1024
        ),
        name="plane_wave_multiples",
    )(*[
        pltpu.with_memory_space_constraint(x, pltpu.HBM)
        for x in (data.reshape(2 * shots, rec_count), receiver_x.reshape(1, rec_count), source_x.reshape(1, src_count))
    ])
    result = ((dot(left, right) + total) * math.sqrt(2.0 / NSLOW)).astype(half)
    return result.reshape(2, shots, rec_count)


def fits(mesh_shape, shots):
    line = mesh_shape["shot"] == len(OWN) and mesh_shape["rep"] == 2
    return line and NSLOW == BLOCKS * BLOCK and shots % 128 == 0


def body(fused, recorded, receiver_x, source_x):
    per_device = recorded.shape[1]
    first_freq = lax.axis_index("freq") * per_device
    outs = []
    for k in range(per_device):
        omega = two_pi * (base_hertz + step_hertz * (first_freq + k).astype(jnp.float32))
        if fused(recorded.shape[2]):
            first_hertz = functools.partial(lambda k, f: f * per_device + k, k)
            outs.append(one_frequency_fused(first_hertz, recorded[:, k], receiver_x, source_x))
        else:
            outs.append(one_frequency(recorded[:, k], receiver_x, source_x, omega))
    return jnp.stack(outs, axis=1)


def solution(mesh):
    return jax.shard_map(
        functools.partial(body, functools.partial(fits, mesh.shape)),
        mesh=mesh,
        in_specs=(P(None, ("parts", "freq"), ("shot", "rep"), None), P("parts"), P("parts")),
        out_specs=P(None, ("parts", "freq"), ("shot", "rep"), None),
        check_vma=False,
    )
```

```python
import functools
import math

import jax
import jax.numpy as jnp
from jax import lax
from jax.experimental import pallas as pl
from jax.experimental.pallas import tpu as pltpu
from jax.sharding import PartitionSpec as P

NSLOW = 1024

two_pi = 6.283185307179586
base_hertz = 40.0
step_hertz = 0.5
slow_max = 0.0005
GROUP = ("shot", "rep")


def angle_table(omega, positions):
    half = NSLOW // 2
    fine = math.gcd(half, 16)
    unit = (omega * (slow_max / NSLOW)) * positions
    coarse = (jnp.arange(half // fine, dtype=jnp.int32) * (2 * fine)).astype(jnp.float32)[:, None] * unit
    small = (2 * jnp.arange(fine, dtype=jnp.int32) + 1).astype(jnp.float32)[:, None] * unit
    cos_a, sin_a = jnp.cos(coarse)[:, None], jnp.sin(coarse)[:, None]
    cos_b, sin_b = jnp.cos(small)[None], jnp.sin(small)[None]
    cosine = cos_a * cos_b - sin_a * sin_b
    sine = sin_a * cos_b + cos_a * sin_b
    return jnp.stack([cosine, sine]).astype(jnp.bfloat16).reshape(NSLOW, positions.shape[0])


def product(form, left, right):
    return jnp.einsum(form, left, right, preferred_element_type=jnp.float32)


def one_frequency(data, receiver_x, source_x, omega):
    shots = data.shape[1]
    src_count, rec_count = source_x.shape[0], receiver_x.shape[0]
    receiver = angle_table(omega, receiver_x)
    source = angle_table(omega, source_x)
    first = lax.axis_index(GROUP) * shots
    mine = angle_table(omega, lax.dynamic_slice_in_dim(source_x, first, shots, 0))
    spread = (product("csr,jr->csj", data, receiver) * math.sqrt(2.0 / rec_count)).astype(jnp.bfloat16)
    met = lax.all_to_all(spread, GROUP, split_axis=2, concat_axis=1, tiled=True)
    plane = (product("qs,csj->cqj", source, met) * math.sqrt(2.0 / src_count)).astype(jnp.bfloat16)
    planes = lax.all_gather(plane, GROUP, axis=2, tiled=True)
    sign = jnp.where(jnp.arange(NSLOW) < NSLOW // 2, 1.0, -1.0) * math.sqrt(2.0 / NSLOW)
    half_way = (product("qs,cqj->csj", mine, planes) * sign).astype(jnp.bfloat16)
    back_real = product("sm,mj->sj", half_way[0], planes[0]) - product("sm,mj->sj", half_way[1], planes[1])
    back_imaginary = product("sm,mj->sj", half_way[0], planes[1]) + product("sm,mj->sj", half_way[1], planes[0])
    back = (jnp.stack([back_real, back_imaginary]) * math.sqrt(1.0 / NSLOW)).astype(jnp.bfloat16)
    return (product("csj,jr->csr", back, receiver) * math.sqrt(2.0 / NSLOW)).astype(jnp.bfloat16)


FINE = 16
HALF = NSLOW // 2
COARSE = HALF // FINE
BLOCK = 128
PAIRS = HALF // BLOCK
PIECES = 4
MESH = pl.DeviceIdType.MESH

OWNER = tuple(2 * s + p % 2 for p in range(PAIRS) for s in range(2))
OWN = tuple(tuple(nb for nb, owner in enumerate(OWNER) if owner == at) for at in range(4))
ORDER = (
    (0, 2, 4, 6, 1, 5, 3, 7),
    (2, 6, 1, 0, 5, 4, 3, 7),
    (1, 5, 2, 3, 6, 7, 0, 4),
    (3, 1, 7, 5, 2, 6, 0, 4),
)
SENDING = (
    (0, 1, 2, 3, 4, 5, 6, 7),
    (0, 1, 4, 3, 5, 7, 2, 6),
    (2, 3, 0, 7, 6, 4, 1, 5),
    (2, 3, 0, 1, 6, 7, 4, 5),
)
BLOCKS = len(OWNER)


def fill_factors(omega, positions, factors, fine, first, rows):
    count = positions.shape[1]
    tile = math.gcd(count, 256)
    sines = [(-1.0) ** n / math.factorial(2 * n + 1) for n in range(7)]
    cosines = [(-1.0) ** n / math.factorial(2 * n) for n in range(8)]
    turn_high = 6.28125
    turn_low = two_pi - turn_high

    def step(i, carry):
        lanes = pl.ds(pl.multiple_of(i * tile, tile), tile)
        unit = positions[:, lanes] * (omega * (slow_max / NSLOW))
        row = lax.broadcasted_iota(jnp.int32, (fine + rows, tile), 0)
        steps = jnp.where(row < fine, 2 * row + 1, (row - fine + first) * (2 * FINE)).astype(jnp.float32)
        phase = steps * unit
        turns = jnp.floor(phase * (1.0 / two_pi) + 0.5)
        half = 0.5 * ((phase - turns * turn_high) - turns * turn_low)
        square = half * half
        sine, cosine = sines[-1], cosines[-1]
        for term in reversed(sines[:-1]):
            sine = sine * square + term
        for term in reversed(cosines[:-1]):
            cosine = cosine * square + term
        sine = sine * half
        for i, values in enumerate((1.0 - 2.0 * sine * sine, 2.0 * sine * cosine)):
            if fine:
                factors[i, :fine, lanes] = values[:fine]
            factors[i, pl.ds(FINE + first, rows), lanes] = values[fine:]
        return carry

    lax.fori_loop(0, count // tile, step, 0)


def fill_pair(factors, table, p):
    count = table.shape[1]
    tile = math.gcd(count, 512)
    steps = BLOCK // FINE
    for first in range(0, count, tile):
        lanes = slice(first, first + tile)
        cos_b = factors[0, :FINE, lanes]
        sin_b = factors[1, :FINE, lanes]

        def step(a, carry):
            cos_a = factors[0, pl.ds(FINE + p * steps + a, 1), lanes]
            sin_a = factors[1, pl.ds(FINE + p * steps + a, 1), lanes]
            row = pl.multiple_of(2 * BLOCK * p + a * FINE, FINE)
            table[pl.ds(row, FINE), lanes] = (cos_a * cos_b - sin_a * sin_b).astype(jnp.bfloat16)
            table[pl.ds(row + BLOCK, FINE), lanes] = (sin_a * cos_b + cos_a * sin_b).astype(jnp.bfloat16)
            return carry

        lax.fori_loop(0, steps, step, 0, unroll=4)


def dot(left, right):
    return jnp.dot(left, right, preferred_element_type=jnp.float32)


def whole_kernel(
    first_hertz, data_in, receiver_in, source_in, result, last_left, last_right,
    data, receiver_x, source_x, receiver, source, receiver_f, source_f, mine, outgoing, met, planes, half_way,
    total, back, crossed,
    spread_send, spread_recv, plane_send, plane_recv, twin_recv, load_sem,
):
    chips, cores = len(OWN), 2
    coarse = BLOCK // FINE
    group = chips * cores
    shots = data.shape[0] // 2
    z, c = lax.axis_index("shot"), lax.axis_index("rep")
    me = z * cores + c
    side = z // 2
    more_up, more_down = z < chips - 1, z > 0

    def pick(values):
        out = jnp.int32(values[-1])
        for i, value in enumerate(values[:-1]):
            out = jnp.where(z == i, jnp.int32(value), out)
        return out

    packed = pick([sum(nb << (3 * i) for i, nb in enumerate(row)) for row in ORDER])
    sending = pick([sum(nb << (3 * i) for i, nb in enumerate(row)) for row in SENDING])

    def nth(i):
        return lax.rem(packed >> (3 * i), BLOCKS)

    def owner_of(nb):
        return 2 * lax.rem(nb, 2) + lax.rem(nb // 2, 2)

    def block_rows(nb):
        return pl.ds(pl.multiple_of(nb * BLOCK, BLOCK), BLOCK)

    def place(d):
        return {"shot": d // cores, "rep": d % cores}

    loads = [
        pltpu.make_async_copy(src, dst, load_sem.at[i])
        for i, (src, dst) in enumerate(((receiver_in, receiver_x), (data_in, data), (source_in, source_x)))
    ]
    for load in loads:
        load.start()
    barrier = pltpu.get_barrier_semaphore()
    for d in range(group):
        @pl.when(d != me)
        def _():
            pl.semaphore_signal(barrier, inc=1, device_id=place(d), device_id_type=MESH)

    hertz = first_hertz(lax.axis_index("freq")).astype(jnp.float32)
    omega = two_pi * (base_hertz + step_hertz * hertz)
    own_rows = pl.ds(pl.multiple_of(me * shots, shots), shots)

    def put(blocks, h, part):
        part = (part * math.sqrt(2.0 / data.shape[1])).astype(jnp.bfloat16)
        for s, nb in enumerate(blocks):
            piece = part[:, s * BLOCK : (s + 1) * BLOCK]
            here = me == owner_of(nb) * cores + h

            @pl.when(here)
            def _():
                met[nb // 2, own_rows, :] = piece

            @pl.when(jnp.logical_not(here))
            def _():
                outgoing[2 * nb + h] = piece

    def send(blocks, h):
        for k in range(2):
            nb = jnp.where(lax.rem(1 - side + c + k, 2) == 0, *blocks)
            to = owner_of(nb)

            @pl.when((to != z) | (c != h))
            def _():
                pltpu.make_async_remote_copy(
                    src_ref=outgoing.at[2 * nb + h], dst_ref=met.at[nb // 2, own_rows],
                    send_sem=spread_send, recv_sem=spread_recv.at[nb // 2],
                    device_id={"shot": to, "rep": h}, device_id_type=MESH,
                ).start()

    def spread(blocks, rows):
        right = jnp.concatenate([receiver[block_rows(nb), :] for nb in blocks], axis=0)
        return lax.dot_general(data[rows, :], right, (((1,), (1,)), ((), ())), preferred_element_type=jnp.float32)

    loads[0].wait()
    fill_factors(omega, receiver_x, receiver_f, FINE, side * coarse, coarse)
    fill_pair(receiver_f, receiver, side)
    loads[1].wait()
    for step in range(PAIRS):
        blocks = [lax.rem(sending >> (3 * i), BLOCKS) for i in (2 * step, 2 * step + 1)]
        if step == 0:
            for h in range(2):
                put(blocks, h, spread(blocks, slice(h * shots, (h + 1) * shots)))
                if h == 0:
                    pl.semaphore_wait(barrier, group - 1)
                send(blocks, h)
            fill_factors(omega, receiver_x, receiver_f, 0, 0, COARSE)
            fill_pair(receiver_f, receiver, 1 - side)
            fill_pair(receiver_f, receiver, 2 + side)
            continue
        part = spread(blocks, slice(0, 2 * shots))
        for h in range(2):
            put(blocks, h, part[h * shots : (h + 1) * shots])
        for h in range(2):
            send(blocks, h)
        if step == 1:
            fill_pair(receiver_f, receiver, 3 - side)

    loads[2].wait()
    fill_factors(omega, source_x, source_f, FINE, 0, COARSE)
    for p in range(PAIRS):
        fill_pair(source_f, source, p)
    mine[...] = source[:, own_rows].T
    for ref in (half_way, back, crossed, last_left, last_right):
        ref[...] = jnp.zeros_like(ref)
    outer = (z == 0) | (z == chips - 1)

    rows_of = NSLOW // PIECES

    def plane_copy(way, nb, h, piece):
        to = [{"shot": z + 1, "rep": c}, {"shot": z - 1, "rep": c}, {"shot": z, "rep": 1 - c}][way]
        part = planes.at[nb, h, pl.ds(pl.multiple_of(piece * rows_of, rows_of), rows_of)]
        return pltpu.make_async_remote_copy(
            src_ref=part, dst_ref=part, send_sem=plane_send.at[way],
            recv_sem=twin_recv.at[nb] if way == 2 else plane_recv.at[nb, piece],
            device_id=to, device_id_type=MESH,
        )

    def whole_copy(way, blocks, recv_sem):
        part = planes.at[blocks, 0]
        return pltpu.make_async_remote_copy(
            src_ref=part, dst_ref=part, send_sem=plane_send.at[way], recv_sem=recv_sem,
            device_id={"rep": 1 - c}, device_id_type=MESH,
        )

    def each_way(nb, up, down, piece, act):
        @pl.when(up)
        def _():
            act(plane_copy(0, nb, c, piece))

        @pl.when(down)
        def _():
            act(plane_copy(1, nb, c, piece))

        act(plane_copy(2, nb, c, piece))

    def start(copy):
        copy.start()

    def own_slice(nb):
        p = nb // 2
        arrived = met.at[p, pl.ds(0, (group - 1) * shots)]
        pltpu.make_async_remote_copy(
            src_ref=arrived, dst_ref=arrived, send_sem=spread_send, recv_sem=spread_recv.at[p],
            device_id={"rep": 1 - c}, device_id_type=MESH,
        ).wait_recv()

        def rows_step(i, carry):
            rows = pl.ds(pl.multiple_of(i * rows_of, rows_of), rows_of)
            piece = (dot(source[rows, :], met[p]) * math.sqrt(2.0 / source.shape[1])).astype(jnp.bfloat16)
            planes[nb, c, rows, :] = piece
            each_way(nb, more_up, more_down, i, start)
            return carry

        lax.fori_loop(0, PIECES, rows_step, 0)

    def ways(i):
        up = pick([int(OWNER[row[i]] < at and at < chips - 1) for at, row in enumerate(ORDER)]) == 1
        down = pick([int(OWNER[row[i]] > at and at > 0) for at, row in enumerate(ORDER)]) == 1
        return up, down

    def passed_slice(i, nb):
        up, down = ways(i)

        def step(piece, carry):
            plane_copy(0, nb, c, piece).wait_recv()
            each_way(nb, up, down, piece, start)
            return carry

        lax.fori_loop(0, PIECES, step, 0)

    def columns(nb):
        return pl.ds(pl.multiple_of(nb * BLOCK, BLOCK), BLOCK)

    def half_slice(nb):
        whole_copy(2, pl.ds(nb, 1), twin_recv.at[nb]).wait_recv()
        sign = (1 - 2 * lax.rem(nb, 2)).astype(jnp.float32) * math.sqrt(2.0 / NSLOW)
        both = jnp.concatenate([planes[nb, 0], planes[nb, 1]], axis=1)
        part = (dot(mine[...], both) * sign).astype(jnp.bfloat16)
        half_way[:shots, columns(nb)] = part[:, :BLOCK]
        half_way[shots:, columns(nb)] = part[:, BLOCK:]

    def mix(both):
        real = both[:shots, :BLOCK] - both[shots:, BLOCK:]
        return real, both[:shots, BLOCK:] + both[shots:, :BLOCK]

    def back_new(nb):
        both = jnp.concatenate([planes[nb, 0], planes[nb, 1]], axis=1)
        return mix(dot(half_way[...], both))

    def back_more(nb, late):
        both = jnp.concatenate([planes[nb, 0, columns(late), :], planes[nb, 1, columns(late), :]], axis=1)
        real, imaginary = mix(dot(half_way[:, columns(late)], both))
        return total[nb, :shots] + real, total[nb, shots:] + imaginary

    def keep_total(nb, parts):
        total[nb, :shots] = parts[0]
        total[nb, shots:] = parts[1]

    def keep_back(nb, parts):
        back[:shots, columns(nb)] = (parts[0] * math.sqrt(1.0 / NSLOW)).astype(jnp.bfloat16)
        back[shots:, columns(nb)] = (parts[1] * math.sqrt(1.0 / NSLOW)).astype(jnp.bfloat16)

    def add_late(n, keep, keep_new):
        late = nth(n)
        for i in range(n):
            keep(nth(i), back_more(nth(i), late))
        keep_new(late, back_new(late))

    scale_back = math.sqrt(1.0 / NSLOW)
    rec_count = receiver.shape[1]
    tile = math.gcd(rec_count, 512)
    last, before = BLOCKS - 1, BLOCKS - 2

    def lanes_of(i):
        return pl.ds(pl.multiple_of(i * tile, tile), tile)

    def right_side():
        late = nth(last)
        for i in range(before):
            for h in range(2):
                crossed[h * BLOCK : (h + 1) * BLOCK, columns(nth(i))] = planes[nth(i), h, columns(late), :]
        last_right[2 * BLOCK : 3 * BLOCK, :] = receiver[columns(late), :]
        last_right[3 * BLOCK :, :] = receiver[columns(nth(before)), :]

        def step(i, carry):
            part = dot(crossed[...], receiver[:, lanes_of(i)])
            last_right[: 2 * BLOCK, lanes_of(i)] = (part * scale_back).astype(jnp.bfloat16)
            return carry

        lax.fori_loop(0, rec_count // tile, step, 0)

    def left_side():
        late, old = nth(last), nth(before)
        whole_copy(2, pl.ds(late, 1), twin_recv.at[late]).wait_recv()
        both = jnp.concatenate([planes[late, 0], planes[late, 1]], axis=1)
        sign = (1 - 2 * lax.rem(late, 2)).astype(jnp.float32) * math.sqrt(2.0 / NSLOW)
        part = (dot(mine[...], both) * sign).astype(jnp.bfloat16)
        base = dot(half_way[...], both)
        real, imaginary = part[:, :BLOCK], part[:, BLOCK:]
        top = jnp.concatenate([real, imaginary], axis=0)
        last_left[:shots, :BLOCK] = real
        last_left[:shots, BLOCK : 2 * BLOCK] = -imaginary
        last_left[shots:, :BLOCK] = imaginary
        last_left[shots:, BLOCK : 2 * BLOCK] = real

        def rest(nb):
            rows = jnp.concatenate([planes[nb, 0, columns(late), :], planes[nb, 1, columns(late), :]], axis=1)
            return dot(top, rows)

        parts = mix(rest(old))
        for at, parts in (
            (3, (total[old, :shots] + parts[0], total[old, shots:] + parts[1])),
            (2, mix(base + rest(late))),
        ):
            for rows, part in zip((slice(0, shots), slice(shots, 2 * shots)), parts):
                last_left[rows, at * BLOCK : (at + 1) * BLOCK] = (part * scale_back).astype(jnp.bfloat16)

    def result_so_far():
        def step(i, carry):
            result[:, lanes_of(i)] = dot(back[...], receiver[:, lanes_of(i)])
            return carry

        lax.fori_loop(0, rec_count // tile, step, 0)

    for i in range(BLOCKS):
        nb = nth(i)
        owners = [row[i] in own for row, own in zip(ORDER, OWN)]
        mine_now = pick([int(x) for x in owners]) == 1
        if any(owners):
            @pl.when(mine_now)
            def _():
                own_slice(nb)
        if not all(owners):
            @pl.when(jnp.logical_not(mine_now))
            def _():
                passed_slice(i, nb)
        if 0 < i < before:
            half_slice(nth(i - 1))
            add_late(i - 1, keep_total, keep_total)
        if i == before - 1:
            @pl.when(outer)
            def _():
                half_slice(nb)
                add_late(i, keep_total, keep_total)
                right_side()
        if i == before:
            @pl.when(jnp.logical_not(outer))
            def _():
                half_slice(nth(i - 1))
                add_late(i - 1, keep_total, keep_total)

            half_slice(nb)

            @pl.when(outer)
            def _():
                add_late(i, keep_back, keep_total)
                result_so_far()

            @pl.when(jnp.logical_not(outer))
            def _():
                add_late(i, keep_total, keep_total)

    sent = outgoing.at[pl.ds(0, 2 * BLOCKS - len(OWN[0]))]
    pltpu.make_async_remote_copy(
        src_ref=sent, dst_ref=sent, send_sem=spread_send, recv_sem=spread_recv.at[0],
        device_id={"rep": 1 - c}, device_id_type=MESH,
    ).wait_send()

    for at in range(chips):
        counts = [sum(owner <= at for owner in OWNER), sum(owner >= at for owner in OWNER)]

        @pl.when(z == at)
        def _():
            for way, count in enumerate(counts):
                if count < BLOCKS:
                    whole_copy(way, pl.ds(0, count), twin_recv.at[0]).wait_send()

    @pl.when(outer)
    def _():
        left_side()

    @pl.when(jnp.logical_not(outer))
    def _():
        half_slice(nth(last))
        add_late(last, keep_back, keep_back)
        result_so_far()

    whole_copy(2, pl.ds(0, BLOCKS), twin_recv.at[0]).wait_send()


def finish_kernel(total, left, right, out, staged, sems):
    rec_count = total.shape[1]
    tile = math.gcd(rec_count, 256)
    copies = []
    for i in range(rec_count // tile):
        lanes = slice(i * tile, (i + 1) * tile)
        part = (dot(left[...], right[:, lanes]) + total[:, lanes]) * math.sqrt(2.0 / NSLOW)
        staged[:, lanes] = part.astype(jnp.bfloat16)
        copies.append(pltpu.make_async_copy(staged.at[:, lanes], out.at[:, lanes], sems.at[i]))
        copies[-1].start()
    for copy in copies:
        copy.wait()


def one_frequency_fused(first_hertz, data, receiver_x, source_x):
    shots, rec_count = data.shape[1:]
    src_count = source_x.shape[0]
    group = 2 * len(OWN)
    vmem = pl.BlockSpec(memory_space=pltpu.VMEM)
    half = jnp.bfloat16
    total, left, right = pl.pallas_call(
        functools.partial(whole_kernel, first_hertz),
        out_shape=(
            jax.ShapeDtypeStruct((2 * shots, rec_count), jnp.float32),
            jax.ShapeDtypeStruct((2 * shots, 4 * BLOCK), half),
            jax.ShapeDtypeStruct((4 * BLOCK, rec_count), half),
        ),
        in_specs=[pl.BlockSpec(memory_space=pltpu.HBM)] * 3,
        out_specs=(vmem, vmem, vmem),
        scratch_shapes=[
            pltpu.VMEM((2 * shots, rec_count), half),
            pltpu.VMEM((1, rec_count), jnp.float32),
            pltpu.VMEM((1, src_count), jnp.float32),
            pltpu.VMEM((NSLOW, rec_count), half),
            pltpu.VMEM((NSLOW, src_count), half),
            pltpu.VMEM((2, COARSE + FINE, rec_count), jnp.float32),
            pltpu.VMEM((2, COARSE + FINE, src_count), jnp.float32),
            pltpu.VMEM((shots, NSLOW), half),
            pltpu.VMEM((2 * BLOCKS, shots, BLOCK), half),
            pltpu.VMEM((PAIRS, src_count, BLOCK), half),
            pltpu.VMEM((BLOCKS, 2, NSLOW, BLOCK), half),
            pltpu.VMEM((2 * shots, NSLOW), half),
            pltpu.VMEM((BLOCKS, 2 * shots, BLOCK), jnp.float32),
            pltpu.VMEM((2 * shots, NSLOW), half),
            pltpu.VMEM((2 * BLOCK, NSLOW), half),
            pltpu.SemaphoreType.DMA,
            pltpu.SemaphoreType.DMA((PAIRS,)),
            pltpu.SemaphoreType.DMA((3,)),
            pltpu.SemaphoreType.DMA((BLOCKS, PIECES)),
            pltpu.SemaphoreType.DMA((BLOCKS,)),
            pltpu.SemaphoreType.DMA((3,)),
        ],
        compiler_params=pltpu.CompilerParams(
            collective_id=0, has_side_effects=True, vmem_limit_bytes=30 * 1024 * 1024
        ),
        name="plane_wave_multiples",
    )(*[
        pltpu.with_memory_space_constraint(x, pltpu.HBM)
        for x in (data.reshape(2 * shots, rec_count), receiver_x.reshape(1, rec_count), source_x.reshape(1, src_count))
    ])
    result = pl.pallas_call(
        finish_kernel,
        out_shape=jax.ShapeDtypeStruct((2 * shots, rec_count), half),
        in_specs=[vmem] * 3,
        out_specs=pl.BlockSpec(memory_space=pl.ANY),
        scratch_shapes=[
            pltpu.VMEM((2 * shots, rec_count), half),
            pltpu.SemaphoreType.DMA((rec_count // math.gcd(rec_count, 256),)),
        ],
        compiler_params=pltpu.CompilerParams(vmem_limit_bytes=24 * 1024 * 1024),
        name="last_block",
    )(total, left, right)
    return result.reshape(2, shots, rec_count)


def fits(mesh_shape, shots):
    line = mesh_shape["shot"] == len(OWN) and mesh_shape["rep"] == 2
    return line and NSLOW == BLOCKS * BLOCK and shots % 128 == 0


def body(fused, recorded, receiver_x, source_x):
    per_device = recorded.shape[1]
    first_freq = lax.axis_index("freq") * per_device
    outs = []
    for k in range(per_device):
        omega = two_pi * (base_hertz + step_hertz * (first_freq + k).astype(jnp.float32))
        if fused(recorded.shape[2]):
            first_hertz = functools.partial(lambda k, f: f * per_device + k, k)
            outs.append(one_frequency_fused(first_hertz, recorded[:, k], receiver_x, source_x))
        else:
            outs.append(one_frequency(recorded[:, k], receiver_x, source_x, omega))
    return jnp.stack(outs, axis=1)


def solution(mesh):
    return jax.shard_map(
        functools.partial(body, functools.partial(fits, mesh.shape)),
        mesh=mesh,
        in_specs=(P(None, ("parts", "freq"), ("shot", "rep"), None), P("parts"), P("parts")),
        out_specs=P(None, ("parts", "freq"), ("shot", "rep"), None),
        check_vma=False,
    )
```

```python
import functools
import math

import jax
import jax.numpy as jnp
from jax import lax
from jax.experimental import pallas as pl
from jax.experimental.pallas import tpu as pltpu
from jax.sharding import PartitionSpec as P

NSLOW = 1024

two_pi = 6.283185307179586
base_hertz = 40.0
step_hertz = 0.5
slow_max = 0.0005
GROUP = ("shot", "rep")


def angle_table(omega, positions):
    half = NSLOW // 2
    fine = math.gcd(half, 16)
    unit = (omega * (slow_max / NSLOW)) * positions
    coarse = (jnp.arange(half // fine, dtype=jnp.int32) * (2 * fine)).astype(jnp.float32)[:, None] * unit
    small = (2 * jnp.arange(fine, dtype=jnp.int32) + 1).astype(jnp.float32)[:, None] * unit
    cos_a, sin_a = jnp.cos(coarse)[:, None], jnp.sin(coarse)[:, None]
    cos_b, sin_b = jnp.cos(small)[None], jnp.sin(small)[None]
    cosine = cos_a * cos_b - sin_a * sin_b
    sine = sin_a * cos_b + cos_a * sin_b
    return jnp.stack([cosine, sine]).astype(jnp.bfloat16).reshape(NSLOW, positions.shape[0])


def product(form, left, right):
    return jnp.einsum(form, left, right, preferred_element_type=jnp.float32)


def one_frequency(data, receiver_x, source_x, omega):
    shots = data.shape[1]
    src_count, rec_count = source_x.shape[0], receiver_x.shape[0]
    receiver = angle_table(omega, receiver_x)
    source = angle_table(omega, source_x)
    first = lax.axis_index(GROUP) * shots
    mine = angle_table(omega, lax.dynamic_slice_in_dim(source_x, first, shots, 0))
    spread = (product("csr,jr->csj", data, receiver) * math.sqrt(2.0 / rec_count)).astype(jnp.bfloat16)
    met = lax.all_to_all(spread, GROUP, split_axis=2, concat_axis=1, tiled=True)
    plane = (product("qs,csj->cqj", source, met) * math.sqrt(2.0 / src_count)).astype(jnp.bfloat16)
    planes = lax.all_gather(plane, GROUP, axis=2, tiled=True)
    sign = jnp.where(jnp.arange(NSLOW) < NSLOW // 2, 1.0, -1.0) * math.sqrt(2.0 / NSLOW)
    half_way = (product("qs,cqj->csj", mine, planes) * sign).astype(jnp.bfloat16)
    back_real = product("sm,mj->sj", half_way[0], planes[0]) - product("sm,mj->sj", half_way[1], planes[1])
    back_imaginary = product("sm,mj->sj", half_way[0], planes[1]) + product("sm,mj->sj", half_way[1], planes[0])
    back = (jnp.stack([back_real, back_imaginary]) * math.sqrt(1.0 / NSLOW)).astype(jnp.bfloat16)
    return (product("csj,jr->csr", back, receiver) * math.sqrt(2.0 / NSLOW)).astype(jnp.bfloat16)


FINE = 16
HALF = NSLOW // 2
COARSE = HALF // FINE
BLOCK = 128
PAIRS = HALF // BLOCK
PIECES = 4
MESH = pl.DeviceIdType.MESH

OWNER = tuple(2 * s + p % 2 for p in range(PAIRS) for s in range(2))
OWN = tuple(tuple(nb for nb, owner in enumerate(OWNER) if owner == at) for at in range(4))
ORDER = (
    (0, 2, 4, 6, 1, 5, 3, 7),
    (2, 6, 1, 0, 5, 4, 3, 7),
    (1, 5, 2, 3, 6, 7, 0, 4),
    (3, 1, 7, 5, 2, 6, 0, 4),
)
SENDING = (
    (0, 1, 2, 3, 6, 7, 4, 5),
    (0, 1, 4, 3, 2, 6, 5, 7),
    (2, 3, 0, 7, 1, 5, 6, 4),
    (2, 3, 0, 1, 4, 5, 6, 7),
)
BLOCKS = len(OWNER)


def fill_factors(omega, positions, factors, fine, first, rows):
    count = positions.shape[1]
    tile = math.gcd(count, 256)
    sines = [(-1.0) ** n / math.factorial(2 * n + 1) for n in range(7)]
    cosines = [(-1.0) ** n / math.factorial(2 * n) for n in range(8)]
    turn_high = 6.28125
    turn_low = two_pi - turn_high

    def step(i, carry):
        lanes = pl.ds(pl.multiple_of(i * tile, tile), tile)
        unit = positions[:, lanes] * (omega * (slow_max / NSLOW))
        row = lax.broadcasted_iota(jnp.int32, (fine + rows, tile), 0)
        steps = jnp.where(row < fine, 2 * row + 1, (row - fine + first) * (2 * FINE)).astype(jnp.float32)
        phase = steps * unit
        turns = jnp.floor(phase * (1.0 / two_pi) + 0.5)
        half = 0.5 * ((phase - turns * turn_high) - turns * turn_low)
        square = half * half
        sine, cosine = sines[-1], cosines[-1]
        for term in reversed(sines[:-1]):
            sine = sine * square + term
        for term in reversed(cosines[:-1]):
            cosine = cosine * square + term
        sine = sine * half
        for i, values in enumerate((1.0 - 2.0 * sine * sine, 2.0 * sine * cosine)):
            if fine:
                factors[i, :fine, lanes] = values[:fine]
            factors[i, pl.ds(FINE + first, rows), lanes] = values[fine:]
        return carry

    lax.fori_loop(0, count // tile, step, 0)


def fill_pair(factors, table, p):
    count = table.shape[1]
    tile = math.gcd(count, 512)
    steps = BLOCK // FINE
    for first in range(0, count, tile):
        lanes = slice(first, first + tile)
        cos_b = factors[0, :FINE, lanes]
        sin_b = factors[1, :FINE, lanes]

        def step(a, carry):
            cos_a = factors[0, pl.ds(FINE + p * steps + a, 1), lanes]
            sin_a = factors[1, pl.ds(FINE + p * steps + a, 1), lanes]
            row = pl.multiple_of(2 * BLOCK * p + a * FINE, FINE)
            table[pl.ds(row, FINE), lanes] = (cos_a * cos_b - sin_a * sin_b).astype(jnp.bfloat16)
            table[pl.ds(row + BLOCK, FINE), lanes] = (sin_a * cos_b + cos_a * sin_b).astype(jnp.bfloat16)
            return carry

        lax.fori_loop(0, steps, step, 0, unroll=4)


def dot(left, right):
    return jnp.dot(left, right, preferred_element_type=jnp.float32)


def whole_kernel(
    first_hertz, data_in, receiver_in, source_in, result, last_left, last_right,
    data, receiver_x, source_x, receiver, source, receiver_f, source_f, mine, outgoing, met, planes, half_way,
    total, back, crossed,
    spread_send, spread_recv, plane_send, plane_recv, twin_recv, load_sem,
):
    chips, cores = len(OWN), 2
    coarse = BLOCK // FINE
    group = chips * cores
    shots = data.shape[0] // 2
    z, c = lax.axis_index("shot"), lax.axis_index("rep")
    me = z * cores + c
    side = z // 2
    more_up, more_down = z < chips - 1, z > 0

    def pick(values):
        out = jnp.int32(values[-1])
        for i, value in enumerate(values[:-1]):
            out = jnp.where(z == i, jnp.int32(value), out)
        return out

    packed = pick([sum(nb << (3 * i) for i, nb in enumerate(row)) for row in ORDER])
    sending = pick([sum(nb << (3 * i) for i, nb in enumerate(row)) for row in SENDING])

    def nth(i):
        return lax.rem(packed >> (3 * i), BLOCKS)

    def owner_of(nb):
        return 2 * lax.rem(nb, 2) + lax.rem(nb // 2, 2)

    def block_rows(nb):
        return pl.ds(pl.multiple_of(nb * BLOCK, BLOCK), BLOCK)

    def place(d):
        return {"shot": d // cores, "rep": d % cores}

    loads = [
        pltpu.make_async_copy(src, dst, load_sem.at[i])
        for i, (src, dst) in enumerate(((receiver_in, receiver_x), (data_in, data), (source_in, source_x)))
    ]
    for load in loads:
        load.start()
    barrier = pltpu.get_barrier_semaphore()
    for d in range(group):
        @pl.when(d != me)
        def _():
            pl.semaphore_signal(barrier, inc=1, device_id=place(d), device_id_type=MESH)

    hertz = first_hertz(lax.axis_index("freq")).astype(jnp.float32)
    omega = two_pi * (base_hertz + step_hertz * hertz)
    own_rows = pl.ds(pl.multiple_of(me * shots, shots), shots)

    def put(blocks, h, part):
        part = (part * math.sqrt(2.0 / data.shape[1])).astype(jnp.bfloat16)
        for s, nb in enumerate(blocks):
            piece = part[:, s * BLOCK : (s + 1) * BLOCK]
            here = me == owner_of(nb) * cores + h

            @pl.when(here)
            def _():
                met[nb // 2, own_rows, :] = piece

            @pl.when(jnp.logical_not(here))
            def _():
                outgoing[2 * nb + h] = piece

    def send(blocks, h):
        for k in range(2):
            nb = jnp.where(lax.rem(1 - side + c + k, 2) == 0, *blocks)
            to = owner_of(nb)

            @pl.when((to != z) | (c != h))
            def _():
                pltpu.make_async_remote_copy(
                    src_ref=outgoing.at[2 * nb + h], dst_ref=met.at[nb // 2, own_rows],
                    send_sem=spread_send, recv_sem=spread_recv.at[nb // 2],
                    device_id={"shot": to, "rep": h}, device_id_type=MESH,
                ).start()

    def spread(blocks, rows):
        right = jnp.concatenate([receiver[block_rows(nb), :] for nb in blocks], axis=0)
        return lax.dot_general(data[rows, :], right, (((1,), (1,)), ((), ())), preferred_element_type=jnp.float32)

    loads[0].wait()
    fill_factors(omega, receiver_x, receiver_f, FINE, side * coarse, coarse)
    fill_pair(receiver_f, receiver, side)
    loads[1].wait()
    for step in range(PAIRS):
        blocks = [lax.rem(sending >> (3 * i), BLOCKS) for i in (2 * step, 2 * step + 1)]
        if step == 0:
            for h in range(2):
                put(blocks, h, spread(blocks, slice(h * shots, (h + 1) * shots)))
                if h == 0:
                    pl.semaphore_wait(barrier, group - 1)
                send(blocks, h)
            fill_factors(omega, receiver_x, receiver_f, 0, 0, COARSE)
            fill_pair(receiver_f, receiver, 1 - side)
            fill_pair(receiver_f, receiver, 2 + side)
            continue
        part = spread(blocks, slice(0, 2 * shots))
        for h in range(2):
            put(blocks, h, part[h * shots : (h + 1) * shots])
        for h in range(2):
            send(blocks, h)
        if step == 1:
            fill_pair(receiver_f, receiver, 3 - side)

    loads[2].wait()
    fill_factors(omega, source_x, source_f, FINE, 0, COARSE)
    for p in range(PAIRS):
        fill_pair(source_f, source, p)
    mine[...] = source[:, own_rows].T
    for ref in (half_way, back, crossed, last_left, last_right):
        ref[...] = jnp.zeros_like(ref)
    outer = (z == 0) | (z == chips - 1)

    rows_of = NSLOW // PIECES

    def plane_copy(way, nb, h, piece):
        to = [{"shot": z + 1, "rep": c}, {"shot": z - 1, "rep": c}, {"shot": z, "rep": 1 - c}][way]
        part = planes.at[nb, h, pl.ds(pl.multiple_of(piece * rows_of, rows_of), rows_of)]
        return pltpu.make_async_remote_copy(
            src_ref=part, dst_ref=part, send_sem=plane_send.at[way],
            recv_sem=twin_recv.at[nb] if way == 2 else plane_recv.at[nb, piece],
            device_id=to, device_id_type=MESH,
        )

    def whole_copy(way, blocks, recv_sem):
        part = planes.at[blocks, 0]
        return pltpu.make_async_remote_copy(
            src_ref=part, dst_ref=part, send_sem=plane_send.at[way], recv_sem=recv_sem,
            device_id={"rep": 1 - c}, device_id_type=MESH,
        )

    def each_way(nb, up, down, piece, act):
        @pl.when(up)
        def _():
            act(plane_copy(0, nb, c, piece))

        @pl.when(down)
        def _():
            act(plane_copy(1, nb, c, piece))

        act(plane_copy(2, nb, c, piece))

    def start(copy):
        copy.start()

    def own_slice(nb):
        p = nb // 2
        arrived = met.at[p, pl.ds(0, (group - 1) * shots)]
        pltpu.make_async_remote_copy(
            src_ref=arrived, dst_ref=arrived, send_sem=spread_send, recv_sem=spread_recv.at[p],
            device_id={"rep": 1 - c}, device_id_type=MESH,
        ).wait_recv()

        def rows_step(i, carry):
            rows = pl.ds(pl.multiple_of(i * rows_of, rows_of), rows_of)
            piece = (dot(source[rows, :], met[p]) * math.sqrt(2.0 / source.shape[1])).astype(jnp.bfloat16)
            planes[nb, c, rows, :] = piece
            each_way(nb, more_up, more_down, i, start)
            return carry

        lax.fori_loop(0, PIECES, rows_step, 0)

    def ways(i):
        up = pick([int(OWNER[row[i]] < at and at < chips - 1) for at, row in enumerate(ORDER)]) == 1
        down = pick([int(OWNER[row[i]] > at and at > 0) for at, row in enumerate(ORDER)]) == 1
        return up, down

    def passed_slice(i, nb):
        up, down = ways(i)

        def step(piece, carry):
            plane_copy(0, nb, c, piece).wait_recv()
            each_way(nb, up, down, piece, start)
            return carry

        lax.fori_loop(0, PIECES, step, 0)

    def columns(nb):
        return pl.ds(pl.multiple_of(nb * BLOCK, BLOCK), BLOCK)

    def half_slice(nb):
        whole_copy(2, pl.ds(nb, 1), twin_recv.at[nb]).wait_recv()
        sign = (1 - 2 * lax.rem(nb, 2)).astype(jnp.float32) * math.sqrt(2.0 / NSLOW)
        both = jnp.concatenate([planes[nb, 0], planes[nb, 1]], axis=1)
        part = (dot(mine[...], both) * sign).astype(jnp.bfloat16)
        half_way[:shots, columns(nb)] = part[:, :BLOCK]
        half_way[shots:, columns(nb)] = part[:, BLOCK:]

    def mix(both):
        real = both[:shots, :BLOCK] - both[shots:, BLOCK:]
        return real, both[:shots, BLOCK:] + both[shots:, :BLOCK]

    def back_new(nb):
        both = jnp.concatenate([planes[nb, 0], planes[nb, 1]], axis=1)
        return mix(dot(half_way[...], both))

    def back_more(nb, late):
        both = jnp.concatenate([planes[nb, 0, columns(late), :], planes[nb, 1, columns(late), :]], axis=1)
        real, imaginary = mix(dot(half_way[:, columns(late)], both))
        return total[nb, :shots] + real, total[nb, shots:] + imaginary

    def keep_total(nb, parts):
        total[nb, :shots] = parts[0]
        total[nb, shots:] = parts[1]

    def keep_back(nb, parts):
        back[:shots, columns(nb)] = (parts[0] * math.sqrt(1.0 / NSLOW)).astype(jnp.bfloat16)
        back[shots:, columns(nb)] = (parts[1] * math.sqrt(1.0 / NSLOW)).astype(jnp.bfloat16)

    def add_late(n, keep, keep_new):
        late = nth(n)
        for i in range(n):
            keep(nth(i), back_more(nth(i), late))
        keep_new(late, back_new(late))

    scale_back = math.sqrt(1.0 / NSLOW)
    rec_count = receiver.shape[1]
    tile = math.gcd(rec_count, 512)
    last, before = BLOCKS - 1, BLOCKS - 2

    def lanes_of(i):
        return pl.ds(pl.multiple_of(i * tile, tile), tile)

    def right_side():
        late = nth(last)
        for i in range(before):
            for h in range(2):
                crossed[h * BLOCK : (h + 1) * BLOCK, columns(nth(i))] = planes[nth(i), h, columns(late), :]
        last_right[2 * BLOCK : 3 * BLOCK, :] = receiver[columns(late), :]
        last_right[3 * BLOCK :, :] = receiver[columns(nth(before)), :]

        def step(i, carry):
            part = dot(crossed[...], receiver[:, lanes_of(i)])
            last_right[: 2 * BLOCK, lanes_of(i)] = (part * scale_back).astype(jnp.bfloat16)
            return carry

        lax.fori_loop(0, rec_count // tile, step, 0)

    def left_side():
        late, old = nth(last), nth(before)
        whole_copy(2, pl.ds(late, 1), twin_recv.at[late]).wait_recv()
        both = jnp.concatenate([planes[late, 0], planes[late, 1]], axis=1)
        sign = (1 - 2 * lax.rem(late, 2)).astype(jnp.float32) * math.sqrt(2.0 / NSLOW)
        part = (dot(mine[...], both) * sign).astype(jnp.bfloat16)
        base = dot(half_way[...], both)
        real, imaginary = part[:, :BLOCK], part[:, BLOCK:]
        top = jnp.concatenate([real, imaginary], axis=0)
        last_left[:shots, :BLOCK] = real
        last_left[:shots, BLOCK : 2 * BLOCK] = -imaginary
        last_left[shots:, :BLOCK] = imaginary
        last_left[shots:, BLOCK : 2 * BLOCK] = real

        def rest(nb):
            rows = jnp.concatenate([planes[nb, 0, columns(late), :], planes[nb, 1, columns(late), :]], axis=1)
            return dot(top, rows)

        parts = mix(rest(old))
        for at, parts in (
            (3, (total[old, :shots] + parts[0], total[old, shots:] + parts[1])),
            (2, mix(base + rest(late))),
        ):
            for rows, part in zip((slice(0, shots), slice(shots, 2 * shots)), parts):
                last_left[rows, at * BLOCK : (at + 1) * BLOCK] = (part * scale_back).astype(jnp.bfloat16)

    def result_so_far():
        def step(i, carry):
            result[:, lanes_of(i)] = dot(back[...], receiver[:, lanes_of(i)])
            return carry

        lax.fori_loop(0, rec_count // tile, step, 0)

    for i in range(BLOCKS):
        nb = nth(i)
        owners = [row[i] in own for row, own in zip(ORDER, OWN)]
        mine_now = pick([int(x) for x in owners]) == 1
        if any(owners):
            @pl.when(mine_now)
            def _():
                own_slice(nb)
        if not all(owners):
            @pl.when(jnp.logical_not(mine_now))
            def _():
                passed_slice(i, nb)
        if 0 < i < before:
            half_slice(nth(i - 1))
            add_late(i - 1, keep_total, keep_total)
        if i == before - 1:
            @pl.when(outer)
            def _():
                half_slice(nb)
                add_late(i, keep_total, keep_total)
                right_side()
        if i == before:
            @pl.when(jnp.logical_not(outer))
            def _():
                half_slice(nth(i - 1))
                add_late(i - 1, keep_total, keep_total)

            half_slice(nb)

            @pl.when(outer)
            def _():
                add_late(i, keep_back, keep_total)
                result_so_far()

            @pl.when(jnp.logical_not(outer))
            def _():
                add_late(i, keep_total, keep_total)

    sent = outgoing.at[pl.ds(0, 2 * BLOCKS - len(OWN[0]))]
    pltpu.make_async_remote_copy(
        src_ref=sent, dst_ref=sent, send_sem=spread_send, recv_sem=spread_recv.at[0],
        device_id={"rep": 1 - c}, device_id_type=MESH,
    ).wait_send()

    for at in range(chips):
        counts = [sum(owner <= at for owner in OWNER), sum(owner >= at for owner in OWNER)]

        @pl.when(z == at)
        def _():
            for way, count in enumerate(counts):
                if count < BLOCKS:
                    whole_copy(way, pl.ds(0, count), twin_recv.at[0]).wait_send()

    @pl.when(outer)
    def _():
        left_side()

    @pl.when(jnp.logical_not(outer))
    def _():
        half_slice(nth(last))
        add_late(last, keep_back, keep_back)
        result_so_far()

    whole_copy(2, pl.ds(0, BLOCKS), twin_recv.at[0]).wait_send()


def finish_kernel(total, left, right, out, staged, sems):
    rec_count = total.shape[1]
    tile = math.gcd(rec_count, 256)
    copies = []
    for i in range(rec_count // tile):
        lanes = slice(i * tile, (i + 1) * tile)
        part = (dot(left[...], right[:, lanes]) + total[:, lanes]) * math.sqrt(2.0 / NSLOW)
        staged[:, lanes] = part.astype(jnp.bfloat16)
        copies.append(pltpu.make_async_copy(staged.at[:, lanes], out.at[:, lanes], sems.at[i]))
        copies[-1].start()
    for copy in copies:
        copy.wait()


def one_frequency_fused(first_hertz, data, receiver_x, source_x):
    shots, rec_count = data.shape[1:]
    src_count = source_x.shape[0]
    group = 2 * len(OWN)
    vmem = pl.BlockSpec(memory_space=pltpu.VMEM)
    half = jnp.bfloat16
    total, left, right = pl.pallas_call(
        functools.partial(whole_kernel, first_hertz),
        out_shape=(
            jax.ShapeDtypeStruct((2 * shots, rec_count), jnp.float32),
            jax.ShapeDtypeStruct((2 * shots, 4 * BLOCK), half),
            jax.ShapeDtypeStruct((4 * BLOCK, rec_count), half),
        ),
        in_specs=[pl.BlockSpec(memory_space=pltpu.HBM)] * 3,
        out_specs=(vmem, vmem, vmem),
        scratch_shapes=[
            pltpu.VMEM((2 * shots, rec_count), half),
            pltpu.VMEM((1, rec_count), jnp.float32),
            pltpu.VMEM((1, src_count), jnp.float32),
            pltpu.VMEM((NSLOW, rec_count), half),
            pltpu.VMEM((NSLOW, src_count), half),
            pltpu.VMEM((2, COARSE + FINE, rec_count), jnp.float32),
            pltpu.VMEM((2, COARSE + FINE, src_count), jnp.float32),
            pltpu.VMEM((shots, NSLOW), half),
            pltpu.VMEM((2 * BLOCKS, shots, BLOCK), half),
            pltpu.VMEM((PAIRS, src_count, BLOCK), half),
            pltpu.VMEM((BLOCKS, 2, NSLOW, BLOCK), half),
            pltpu.VMEM((2 * shots, NSLOW), half),
            pltpu.VMEM((BLOCKS, 2 * shots, BLOCK), jnp.float32),
            pltpu.VMEM((2 * shots, NSLOW), half),
            pltpu.VMEM((2 * BLOCK, NSLOW), half),
            pltpu.SemaphoreType.DMA,
            pltpu.SemaphoreType.DMA((PAIRS,)),
            pltpu.SemaphoreType.DMA((3,)),
            pltpu.SemaphoreType.DMA((BLOCKS, PIECES)),
            pltpu.SemaphoreType.DMA((BLOCKS,)),
            pltpu.SemaphoreType.DMA((3,)),
        ],
        compiler_params=pltpu.CompilerParams(
            collective_id=0, has_side_effects=True, vmem_limit_bytes=30 * 1024 * 1024
        ),
        name="plane_wave_multiples",
    )(*[
        pltpu.with_memory_space_constraint(x, pltpu.HBM)
        for x in (data.reshape(2 * shots, rec_count), receiver_x.reshape(1, rec_count), source_x.reshape(1, src_count))
    ])
    result = pl.pallas_call(
        finish_kernel,
        out_shape=jax.ShapeDtypeStruct((2 * shots, rec_count), half),
        in_specs=[vmem] * 3,
        out_specs=pl.BlockSpec(memory_space=pl.ANY),
        scratch_shapes=[
            pltpu.VMEM((2 * shots, rec_count), half),
            pltpu.SemaphoreType.DMA((rec_count // math.gcd(rec_count, 256),)),
        ],
        compiler_params=pltpu.CompilerParams(vmem_limit_bytes=24 * 1024 * 1024),
        name="last_block",
    )(total, left, right)
    return result.reshape(2, shots, rec_count)


def fits(mesh_shape, shots):
    line = mesh_shape["shot"] == len(OWN) and mesh_shape["rep"] == 2
    return line and NSLOW == BLOCKS * BLOCK and shots % 128 == 0


def body(fused, recorded, receiver_x, source_x):
    per_device = recorded.shape[1]
    first_freq = lax.axis_index("freq") * per_device
    outs = []
    for k in range(per_device):
        omega = two_pi * (base_hertz + step_hertz * (first_freq + k).astype(jnp.float32))
        if fused(recorded.shape[2]):
            first_hertz = functools.partial(lambda k, f: f * per_device + k, k)
            outs.append(one_frequency_fused(first_hertz, recorded[:, k], receiver_x, source_x))
        else:
            outs.append(one_frequency(recorded[:, k], receiver_x, source_x, omega))
    return jnp.stack(outs, axis=1)


def solution(mesh):
    return jax.shard_map(
        functools.partial(body, functools.partial(fits, mesh.shape)),
        mesh=mesh,
        in_specs=(P(None, ("parts", "freq"), ("shot", "rep"), None), P("parts"), P("parts")),
        out_specs=P(None, ("parts", "freq"), ("shot", "rep"), None),
        check_vma=False,
    )
```

```python
import functools
import math

import jax
import jax.numpy as jnp
from jax import lax
from jax.experimental import pallas as pl
from jax.experimental.pallas import tpu as pltpu
from jax.sharding import PartitionSpec as P

NSLOW = 1024

two_pi = 6.283185307179586
base_hertz = 40.0
step_hertz = 0.5
slow_max = 0.0005
GROUP = ("shot", "rep")


def angle_table(omega, positions):
    half = NSLOW // 2
    fine = math.gcd(half, 16)
    unit = (omega * (slow_max / NSLOW)) * positions
    coarse = (jnp.arange(half // fine, dtype=jnp.int32) * (2 * fine)).astype(jnp.float32)[:, None] * unit
    small = (2 * jnp.arange(fine, dtype=jnp.int32) + 1).astype(jnp.float32)[:, None] * unit
    cos_a, sin_a = jnp.cos(coarse)[:, None], jnp.sin(coarse)[:, None]
    cos_b, sin_b = jnp.cos(small)[None], jnp.sin(small)[None]
    cosine = cos_a * cos_b - sin_a * sin_b
    sine = sin_a * cos_b + cos_a * sin_b
    return jnp.stack([cosine, sine]).astype(jnp.bfloat16).reshape(NSLOW, positions.shape[0])


def product(form, left, right):
    return jnp.einsum(form, left, right, preferred_element_type=jnp.float32)


def one_frequency(data, receiver_x, source_x, omega):
    shots = data.shape[1]
    src_count, rec_count = source_x.shape[0], receiver_x.shape[0]
    receiver = angle_table(omega, receiver_x)
    source = angle_table(omega, source_x)
    first = lax.axis_index(GROUP) * shots
    mine = angle_table(omega, lax.dynamic_slice_in_dim(source_x, first, shots, 0))
    spread = (product("csr,jr->csj", data, receiver) * math.sqrt(2.0 / rec_count)).astype(jnp.bfloat16)
    met = lax.all_to_all(spread, GROUP, split_axis=2, concat_axis=1, tiled=True)
    plane = (product("qs,csj->cqj", source, met) * math.sqrt(2.0 / src_count)).astype(jnp.bfloat16)
    planes = lax.all_gather(plane, GROUP, axis=2, tiled=True)
    sign = jnp.where(jnp.arange(NSLOW) < NSLOW // 2, 1.0, -1.0) * math.sqrt(2.0 / NSLOW)
    half_way = (product("qs,cqj->csj", mine, planes) * sign).astype(jnp.bfloat16)
    back_real = product("sm,mj->sj", half_way[0], planes[0]) - product("sm,mj->sj", half_way[1], planes[1])
    back_imaginary = product("sm,mj->sj", half_way[0], planes[1]) + product("sm,mj->sj", half_way[1], planes[0])
    back = (jnp.stack([back_real, back_imaginary]) * math.sqrt(1.0 / NSLOW)).astype(jnp.bfloat16)
    return (product("csj,jr->csr", back, receiver) * math.sqrt(2.0 / NSLOW)).astype(jnp.bfloat16)


FINE = 16
HALF = NSLOW // 2
COARSE = HALF // FINE
BLOCK = 128
PAIRS = HALF // BLOCK
PIECES = 4
MESH = pl.DeviceIdType.MESH

OWNER = tuple(2 * s + p % 2 for p in range(PAIRS) for s in range(2))
OWN = tuple(tuple(nb for nb, owner in enumerate(OWNER) if owner == at) for at in range(4))
ORDER = (
    (0, 2, 4, 6, 1, 5, 3, 7),
    (2, 6, 1, 0, 5, 4, 3, 7),
    (1, 5, 2, 3, 6, 7, 0, 4),
    (3, 1, 7, 5, 2, 6, 0, 4),
)
SENDING = (
    (0, 1, 2, 3, 4, 5, 6, 7),
    (0, 1, 4, 3, 5, 7, 2, 6),
    (2, 3, 0, 7, 6, 4, 1, 5),
    (2, 3, 0, 1, 6, 7, 4, 5),
)
BLOCKS = len(OWNER)


def fill_factors(omega, positions, factors, fine, first, rows):
    count = positions.shape[1]
    tile = math.gcd(count, 256)
    sines = [(-1.0) ** n / math.factorial(2 * n + 1) for n in range(7)]
    cosines = [(-1.0) ** n / math.factorial(2 * n) for n in range(8)]
    turn_high = 6.28125
    turn_low = two_pi - turn_high

    def step(i, carry):
        lanes = pl.ds(pl.multiple_of(i * tile, tile), tile)
        unit = positions[:, lanes] * (omega * (slow_max / NSLOW))
        row = lax.broadcasted_iota(jnp.int32, (fine + rows, tile), 0)
        steps = jnp.where(row < fine, 2 * row + 1, (row - fine + first) * (2 * FINE)).astype(jnp.float32)
        phase = steps * unit
        turns = jnp.floor(phase * (1.0 / two_pi) + 0.5)
        half = 0.5 * ((phase - turns * turn_high) - turns * turn_low)
        square = half * half
        sine, cosine = sines[-1], cosines[-1]
        for term in reversed(sines[:-1]):
            sine = sine * square + term
        for term in reversed(cosines[:-1]):
            cosine = cosine * square + term
        sine = sine * half
        for i, values in enumerate((1.0 - 2.0 * sine * sine, 2.0 * sine * cosine)):
            if fine:
                factors[i, :fine, lanes] = values[:fine]
            factors[i, pl.ds(FINE + first, rows), lanes] = values[fine:]
        return carry

    lax.fori_loop(0, count // tile, step, 0)


def fill_pair(factors, table, p):
    count = table.shape[1]
    tile = math.gcd(count, 512)
    steps = BLOCK // FINE
    for first in range(0, count, tile):
        lanes = slice(first, first + tile)
        cos_b = factors[0, :FINE, lanes]
        sin_b = factors[1, :FINE, lanes]

        def step(a, carry):
            cos_a = factors[0, pl.ds(FINE + p * steps + a, 1), lanes]
            sin_a = factors[1, pl.ds(FINE + p * steps + a, 1), lanes]
            row = pl.multiple_of(2 * BLOCK * p + a * FINE, FINE)
            table[pl.ds(row, FINE), lanes] = (cos_a * cos_b - sin_a * sin_b).astype(jnp.bfloat16)
            table[pl.ds(row + BLOCK, FINE), lanes] = (sin_a * cos_b + cos_a * sin_b).astype(jnp.bfloat16)
            return carry

        lax.fori_loop(0, steps, step, 0, unroll=4)


def dot(left, right):
    return jnp.dot(left, right, preferred_element_type=jnp.float32)


def whole_kernel(
    first_hertz, data_in, receiver_in, source_in, result, last_left, last_right,
    data, receiver_x, source_x, receiver, source, receiver_f, source_f, mine, outgoing, met, planes, half_way,
    total, back, crossed,
    spread_send, spread_recv, plane_send, plane_recv, twin_recv, load_sem,
):
    chips, cores = len(OWN), 2
    coarse = BLOCK // FINE
    group = chips * cores
    shots = data.shape[0] // 2
    z, c = lax.axis_index("shot"), lax.axis_index("rep")
    me = z * cores + c
    side = z // 2
    more_up, more_down = z < chips - 1, z > 0

    def pick(values):
        out = jnp.int32(values[-1])
        for i, value in enumerate(values[:-1]):
            out = jnp.where(z == i, jnp.int32(value), out)
        return out

    packed = pick([sum(nb << (3 * i) for i, nb in enumerate(row)) for row in ORDER])
    sending = pick([sum(nb << (3 * i) for i, nb in enumerate(row)) for row in SENDING])

    def nth(i):
        return lax.rem(packed >> (3 * i), BLOCKS)

    def owner_of(nb):
        return 2 * lax.rem(nb, 2) + lax.rem(nb // 2, 2)

    def block_rows(nb):
        return pl.ds(pl.multiple_of(nb * BLOCK, BLOCK), BLOCK)

    def place(d):
        return {"shot": d // cores, "rep": d % cores}

    loads = [
        pltpu.make_async_copy(src, dst, load_sem.at[i])
        for i, (src, dst) in enumerate(((receiver_in, receiver_x), (data_in, data), (source_in, source_x)))
    ]
    for load in loads:
        load.start()
    barrier = pltpu.get_barrier_semaphore()
    for d in range(group):
        @pl.when(d != me)
        def _():
            pl.semaphore_signal(barrier, inc=1, device_id=place(d), device_id_type=MESH)

    hertz = first_hertz(lax.axis_index("freq")).astype(jnp.float32)
    omega = two_pi * (base_hertz + step_hertz * hertz)
    own_rows = pl.ds(pl.multiple_of(me * shots, shots), shots)

    def put(blocks, h, part):
        part = (part * math.sqrt(2.0 / data.shape[1])).astype(jnp.bfloat16)
        for s, nb in enumerate(blocks):
            piece = part[:, s * BLOCK : (s + 1) * BLOCK]
            here = me == owner_of(nb) * cores + h

            @pl.when(here)
            def _():
                met[nb // 2, own_rows, :] = piece

            @pl.when(jnp.logical_not(here))
            def _():
                outgoing[2 * nb + h] = piece

    def send(blocks, h):
        for k in range(2):
            nb = jnp.where(lax.rem(1 - side + c + k, 2) == 0, *blocks)
            to = owner_of(nb)

            @pl.when((to != z) | (c != h))
            def _():
                pltpu.make_async_remote_copy(
                    src_ref=outgoing.at[2 * nb + h], dst_ref=met.at[nb // 2, own_rows],
                    send_sem=spread_send, recv_sem=spread_recv.at[nb // 2],
                    device_id={"shot": to, "rep": h}, device_id_type=MESH,
                ).start()

    def spread(blocks, rows):
        right = jnp.concatenate([receiver[block_rows(nb), :] for nb in blocks], axis=0)
        return lax.dot_general(data[rows, :], right, (((1,), (1,)), ((), ())), preferred_element_type=jnp.float32)

    loads[0].wait()
    fill_factors(omega, receiver_x, receiver_f, FINE, side * coarse, coarse)
    fill_pair(receiver_f, receiver, side)
    loads[1].wait()
    for step in range(PAIRS):
        blocks = [lax.rem(sending >> (3 * i), BLOCKS) for i in (2 * step, 2 * step + 1)]
        if step == 0:
            for h in range(2):
                put(blocks, h, spread(blocks, slice(h * shots, (h + 1) * shots)))
                if h == 0:
                    pl.semaphore_wait(barrier, group - 1)
                send(blocks, h)
            fill_factors(omega, receiver_x, receiver_f, 0, 0, COARSE)
            fill_pair(receiver_f, receiver, 1 - side)
            fill_pair(receiver_f, receiver, 2 + side)
            continue
        part = spread(blocks, slice(0, 2 * shots))
        for h in range(2):
            put(blocks, h, part[h * shots : (h + 1) * shots])
        for h in range(2):
            send(blocks, h)
        if step == 1:
            fill_pair(receiver_f, receiver, 3 - side)

    loads[2].wait()
    fill_factors(omega, source_x, source_f, FINE, 0, COARSE)
    for p in range(PAIRS):
        fill_pair(source_f, source, p)
    mine[...] = source[:, own_rows].T
    for ref in (half_way, back, crossed, last_left, last_right):
        ref[...] = jnp.zeros_like(ref)
    outer = (z == 0) | (z == chips - 1)

    rows_of = NSLOW // PIECES

    def plane_copy(way, nb, h, piece):
        to = [{"shot": z + 1, "rep": c}, {"shot": z - 1, "rep": c}, {"shot": z, "rep": 1 - c}][way]
        part = planes.at[nb, h, pl.ds(pl.multiple_of(piece * rows_of, rows_of), rows_of)]
        return pltpu.make_async_remote_copy(
            src_ref=part, dst_ref=part, send_sem=plane_send.at[way],
            recv_sem=twin_recv.at[nb] if way == 2 else plane_recv.at[nb, piece],
            device_id=to, device_id_type=MESH,
        )

    def whole_copy(way, blocks, recv_sem):
        part = planes.at[blocks, 0]
        return pltpu.make_async_remote_copy(
            src_ref=part, dst_ref=part, send_sem=plane_send.at[way], recv_sem=recv_sem,
            device_id={"rep": 1 - c}, device_id_type=MESH,
        )

    def each_way(nb, up, down, piece, act):
        @pl.when(up)
        def _():
            act(plane_copy(0, nb, c, piece))

        @pl.when(down)
        def _():
            act(plane_copy(1, nb, c, piece))

        act(plane_copy(2, nb, c, piece))

    def start(copy):
        copy.start()

    def own_slice(nb):
        p = nb // 2
        arrived = met.at[p, pl.ds(0, (group - 1) * shots)]
        pltpu.make_async_remote_copy(
            src_ref=arrived, dst_ref=arrived, send_sem=spread_send, recv_sem=spread_recv.at[p],
            device_id={"rep": 1 - c}, device_id_type=MESH,
        ).wait_recv()

        def rows_step(i, carry):
            rows = pl.ds(pl.multiple_of(i * rows_of, rows_of), rows_of)
            piece = (dot(source[rows, :], met[p]) * math.sqrt(2.0 / source.shape[1])).astype(jnp.bfloat16)
            planes[nb, c, rows, :] = piece
            each_way(nb, more_up, more_down, i, start)
            return carry

        lax.fori_loop(0, PIECES, rows_step, 0)

    def ways(i):
        up = pick([int(OWNER[row[i]] < at and at < chips - 1) for at, row in enumerate(ORDER)]) == 1
        down = pick([int(OWNER[row[i]] > at and at > 0) for at, row in enumerate(ORDER)]) == 1
        return up, down

    def passed_slice(i, nb):
        up, down = ways(i)

        def step(piece, carry):
            plane_copy(0, nb, c, piece).wait_recv()
            each_way(nb, up, down, piece, start)
            return carry

        lax.fori_loop(0, PIECES, step, 0)

    def columns(nb):
        return pl.ds(pl.multiple_of(nb * BLOCK, BLOCK), BLOCK)

    def half_slice(nb):
        whole_copy(2, pl.ds(nb, 1), twin_recv.at[nb]).wait_recv()
        sign = (1 - 2 * lax.rem(nb, 2)).astype(jnp.float32) * math.sqrt(2.0 / NSLOW)
        both = jnp.concatenate([planes[nb, 0], planes[nb, 1]], axis=1)
        part = (dot(mine[...], both) * sign).astype(jnp.bfloat16)
        half_way[:shots, columns(nb)] = part[:, :BLOCK]
        half_way[shots:, columns(nb)] = part[:, BLOCK:]

    def mix(both):
        real = both[:shots, :BLOCK] - both[shots:, BLOCK:]
        return real, both[:shots, BLOCK:] + both[shots:, :BLOCK]

    def back_new(nb):
        both = jnp.concatenate([planes[nb, 0], planes[nb, 1]], axis=1)
        return mix(dot(half_way[...], both))

    def back_more(nb, late):
        both = jnp.concatenate([planes[nb, 0, columns(late), :], planes[nb, 1, columns(late), :]], axis=1)
        real, imaginary = mix(dot(half_way[:, columns(late)], both))
        return total[nb, :shots] + real, total[nb, shots:] + imaginary

    def keep_total(nb, parts):
        total[nb, :shots] = parts[0]
        total[nb, shots:] = parts[1]

    def keep_back(nb, parts):
        back[:shots, columns(nb)] = (parts[0] * math.sqrt(1.0 / NSLOW)).astype(jnp.bfloat16)
        back[shots:, columns(nb)] = (parts[1] * math.sqrt(1.0 / NSLOW)).astype(jnp.bfloat16)

    def add_late(n, keep, keep_new):
        late = nth(n)
        for i in range(n):
            keep(nth(i), back_more(nth(i), late))
        keep_new(late, back_new(late))

    scale_back = math.sqrt(1.0 / NSLOW)
    rec_count = receiver.shape[1]
    tile = math.gcd(rec_count, 512)
    last, before = BLOCKS - 1, BLOCKS - 2

    def lanes_of(i):
        return pl.ds(pl.multiple_of(i * tile, tile), tile)

    def right_side():
        late = nth(last)
        for i in range(before):
            for h in range(2):
                crossed[h * BLOCK : (h + 1) * BLOCK, columns(nth(i))] = planes[nth(i), h, columns(late), :]
        last_right[2 * BLOCK : 3 * BLOCK, :] = receiver[columns(late), :]
        last_right[3 * BLOCK :, :] = receiver[columns(nth(before)), :]

        def step(i, carry):
            part = dot(crossed[...], receiver[:, lanes_of(i)])
            last_right[: 2 * BLOCK, lanes_of(i)] = (part * scale_back).astype(jnp.bfloat16)
            return carry

        lax.fori_loop(0, rec_count // tile, step, 0)

    def left_side():
        late, old = nth(last), nth(before)
        whole_copy(2, pl.ds(late, 1), twin_recv.at[late]).wait_recv()
        both = jnp.concatenate([planes[late, 0], planes[late, 1]], axis=1)
        sign = (1 - 2 * lax.rem(late, 2)).astype(jnp.float32) * math.sqrt(2.0 / NSLOW)
        part = (dot(mine[...], both) * sign).astype(jnp.bfloat16)
        base = dot(half_way[...], both)
        real, imaginary = part[:, :BLOCK], part[:, BLOCK:]
        top = jnp.concatenate([real, imaginary], axis=0)
        last_left[:shots, :BLOCK] = real
        last_left[:shots, BLOCK : 2 * BLOCK] = -imaginary
        last_left[shots:, :BLOCK] = imaginary
        last_left[shots:, BLOCK : 2 * BLOCK] = real

        def rest(nb):
            rows = jnp.concatenate([planes[nb, 0, columns(late), :], planes[nb, 1, columns(late), :]], axis=1)
            return dot(top, rows)

        parts = mix(rest(old))
        for at, parts in (
            (3, (total[old, :shots] + parts[0], total[old, shots:] + parts[1])),
            (2, mix(base + rest(late))),
        ):
            for rows, part in zip((slice(0, shots), slice(shots, 2 * shots)), parts):
                last_left[rows, at * BLOCK : (at + 1) * BLOCK] = (part * scale_back).astype(jnp.bfloat16)

    def result_so_far():
        def step(i, carry):
            result[:, lanes_of(i)] = dot(back[...], receiver[:, lanes_of(i)]).astype(jnp.bfloat16)
            return carry

        lax.fori_loop(0, rec_count // tile, step, 0)

    for i in range(BLOCKS):
        nb = nth(i)
        owners = [row[i] in own for row, own in zip(ORDER, OWN)]
        mine_now = pick([int(x) for x in owners]) == 1
        if any(owners):
            @pl.when(mine_now)
            def _():
                own_slice(nb)
        if not all(owners):
            @pl.when(jnp.logical_not(mine_now))
            def _():
                passed_slice(i, nb)
        if 0 < i < before:
            half_slice(nth(i - 1))
            add_late(i - 1, keep_total, keep_total)
        if i == before - 1:
            @pl.when(outer)
            def _():
                half_slice(nb)
                add_late(i, keep_total, keep_total)
                right_side()
        if i == before:
            @pl.when(jnp.logical_not(outer))
            def _():
                half_slice(nth(i - 1))
                add_late(i - 1, keep_total, keep_total)

            half_slice(nb)

            @pl.when(outer)
            def _():
                add_late(i, keep_back, keep_total)
                result_so_far()

            @pl.when(jnp.logical_not(outer))
            def _():
                add_late(i, keep_total, keep_total)

    sent = outgoing.at[pl.ds(0, 2 * BLOCKS - len(OWN[0]))]
    pltpu.make_async_remote_copy(
        src_ref=sent, dst_ref=sent, send_sem=spread_send, recv_sem=spread_recv.at[0],
        device_id={"rep": 1 - c}, device_id_type=MESH,
    ).wait_send()

    for at in range(chips):
        counts = [sum(owner <= at for owner in OWNER), sum(owner >= at for owner in OWNER)]

        @pl.when(z == at)
        def _():
            for way, count in enumerate(counts):
                if count < BLOCKS:
                    whole_copy(way, pl.ds(0, count), twin_recv.at[0]).wait_send()

    @pl.when(outer)
    def _():
        left_side()

    @pl.when(jnp.logical_not(outer))
    def _():
        half_slice(nth(last))
        add_late(last, keep_back, keep_back)
        result_so_far()

    whole_copy(2, pl.ds(0, BLOCKS), twin_recv.at[0]).wait_send()


def finish_kernel(total, left, right, out, staged, sems):
    rec_count = total.shape[1]
    tile = math.gcd(rec_count, 256)
    copies = []
    for i in range(rec_count // tile):
        lanes = slice(i * tile, (i + 1) * tile)
        part = (dot(left[...], right[:, lanes]) + total[:, lanes]) * math.sqrt(2.0 / NSLOW)
        staged[:, lanes] = part.astype(jnp.bfloat16)
        copies.append(pltpu.make_async_copy(staged.at[:, lanes], out.at[:, lanes], sems.at[i]))
        copies[-1].start()
    for copy in copies:
        copy.wait()


def one_frequency_fused(first_hertz, data, receiver_x, source_x):
    shots, rec_count = data.shape[1:]
    src_count = source_x.shape[0]
    group = 2 * len(OWN)
    vmem = pl.BlockSpec(memory_space=pltpu.VMEM)
    half = jnp.bfloat16
    total, left, right = pl.pallas_call(
        functools.partial(whole_kernel, first_hertz),
        out_shape=(
            jax.ShapeDtypeStruct((2 * shots, rec_count), half),
            jax.ShapeDtypeStruct((2 * shots, 4 * BLOCK), half),
            jax.ShapeDtypeStruct((4 * BLOCK, rec_count), half),
        ),
        in_specs=[pl.BlockSpec(memory_space=pltpu.HBM)] * 3,
        out_specs=(vmem, vmem, vmem),
        scratch_shapes=[
            pltpu.VMEM((2 * shots, rec_count), half),
            pltpu.VMEM((1, rec_count), jnp.float32),
            pltpu.VMEM((1, src_count), jnp.float32),
            pltpu.VMEM((NSLOW, rec_count), half),
            pltpu.VMEM((NSLOW, src_count), half),
            pltpu.VMEM((2, COARSE + FINE, rec_count), jnp.float32),
            pltpu.VMEM((2, COARSE + FINE, src_count), jnp.float32),
            pltpu.VMEM((shots, NSLOW), half),
            pltpu.VMEM((2 * BLOCKS, shots, BLOCK), half),
            pltpu.VMEM((PAIRS, src_count, BLOCK), half),
            pltpu.VMEM((BLOCKS, 2, NSLOW, BLOCK), half),
            pltpu.VMEM((2 * shots, NSLOW), half),
            pltpu.VMEM((BLOCKS, 2 * shots, BLOCK), jnp.float32),
            pltpu.VMEM((2 * shots, NSLOW), half),
            pltpu.VMEM((2 * BLOCK, NSLOW), half),
            pltpu.SemaphoreType.DMA,
            pltpu.SemaphoreType.DMA((PAIRS,)),
            pltpu.SemaphoreType.DMA((3,)),
            pltpu.SemaphoreType.DMA((BLOCKS, PIECES)),
            pltpu.SemaphoreType.DMA((BLOCKS,)),
            pltpu.SemaphoreType.DMA((3,)),
        ],
        compiler_params=pltpu.CompilerParams(
            collective_id=0, has_side_effects=True, vmem_limit_bytes=30 * 1024 * 1024
        ),
        name="plane_wave_multiples",
    )(*[
        pltpu.with_memory_space_constraint(x, pltpu.HBM)
        for x in (data.reshape(2 * shots, rec_count), receiver_x.reshape(1, rec_count), source_x.reshape(1, src_count))
    ])
    result = pl.pallas_call(
        finish_kernel,
        out_shape=jax.ShapeDtypeStruct((2 * shots, rec_count), half),
        in_specs=[vmem] * 3,
        out_specs=pl.BlockSpec(memory_space=pl.ANY),
        scratch_shapes=[
            pltpu.VMEM((2 * shots, rec_count), half),
            pltpu.SemaphoreType.DMA((rec_count // math.gcd(rec_count, 256),)),
        ],
        compiler_params=pltpu.CompilerParams(vmem_limit_bytes=24 * 1024 * 1024),
        name="last_block",
    )(total, left, right)
    return result.reshape(2, shots, rec_count)


def fits(mesh_shape, shots):
    line = mesh_shape["shot"] == len(OWN) and mesh_shape["rep"] == 2
    return line and NSLOW == BLOCKS * BLOCK and shots % 128 == 0


def body(fused, recorded, receiver_x, source_x):
    per_device = recorded.shape[1]
    first_freq = lax.axis_index("freq") * per_device
    outs = []
    for k in range(per_device):
        omega = two_pi * (base_hertz + step_hertz * (first_freq + k).astype(jnp.float32))
        if fused(recorded.shape[2]):
            first_hertz = functools.partial(lambda k, f: f * per_device + k, k)
            outs.append(one_frequency_fused(first_hertz, recorded[:, k], receiver_x, source_x))
        else:
            outs.append(one_frequency(recorded[:, k], receiver_x, source_x, omega))
    return jnp.stack(outs, axis=1)


def solution(mesh):
    return jax.shard_map(
        functools.partial(body, functools.partial(fits, mesh.shape)),
        mesh=mesh,
        in_specs=(P(None, ("parts", "freq"), ("shot", "rep"), None), P("parts"), P("parts")),
        out_specs=P(None, ("parts", "freq"), ("shot", "rep"), None),
        check_vma=False,
    )
```
